32 devices in a mesh: gx: 4 (over x, core), gy: 8 (over z, y).
Axes of the slice: x: 2, y: 2, z: 4, core: 2. Of those that a mesh axis runs over, the one named last changes fastest.
Arguments:
- features: bfloat16 [8192, 128], P(('gx', 'gy')), may hold values from -6 to 6
- tile_vals: bfloat16 [2048, 128, 128], P(('gx', 'gy')), may hold values from -0.125 to 0.125
- tile_row: int32 [2048], P(('gx', 'gy')), may hold values from 0 to 63, as said below
- tile_col: int32 [2048], P(('gx', 'gy')), may hold values from 0 to 63, as said below
- tile_work: int32 [2048], P(('gx', 'gy')), may hold values from 0 to 16384, as said below
Outputs:
- product: float32 [8192, 128], P(('gx', 'gy'))
- moved_vals: bfloat16 [1024, 128, 128], P(('gx', 'gy'))
- moved_row: int32 [1024], P(('gx', 'gy'))
- moved_col: int32 [1024], P(('gx', 'gy'))
- moved_work: int32 [1024], P(('gx', 'gy'))
The draws below stay inside these ranges and needn't reach their ends.
Inputs may be any that keep to these rules, and one draw needn't show every extreme that they name: `tile_work`: on every device the live slots come first; each gx row of 8 devices holds exactly 256 live tiles, and in every row one device has all 64 slots live. `tile_row`: A tile held by device (a, b) has a row block owned by a device of gx index a. `tile_col`: A tile held by device (a, b) has a column block owned by a device of gy index b.
All inputs are finite; a program needn't handle non-finite values.
Results may differ from the reference program's by a relative error of at most 0.001.
Values may be sent and summed in bfloat16 or wider, within the bound.
A program may use at most 64 MiB of HBM per device.

```python
import jax
import jax.numpy as jnp
from jax import lax

B = 128
K = 128
VBD = 2
TD = 64
OWN = 32
NB = 64
NV = 8192
NT = 2048
N_GX = 4
N_GY = 8


def skewed_index(key, shape, extent):
    first = jax.random.randint(jax.random.fold_in(key, 11), shape, 0, extent)
    second = jax.random.randint(jax.random.fold_in(key, 12), shape, 0, extent)
    rotate = jax.random.randint(jax.random.fold_in(key, 13), (), 0, extent)
    return (first * second // extent + rotate) % extent


def draw_tile_work(key, part):
    half = N_GY // 2
    delta = jax.random.randint(jax.random.fold_in(key, 1), (N_GX, half), 1 - OWN, OWN)
    forced = jax.random.randint(jax.random.fold_in(key, 2), (N_GX,), 0, half)
    delta = jnp.where(jnp.arange(half)[None, :] == forced[:, None], OWN, delta)
    paired = jnp.concatenate([OWN + delta, OWN - delta], axis=1)
    row_keys = jax.random.split(jax.random.fold_in(key, 3), N_GX)
    counts = jax.vmap(lambda row_key, row: jax.random.permutation(row_key, row))(row_keys, paired)
    slot = jnp.arange(TD, dtype=jnp.int32)[None, None, :]
    amounts = jax.random.randint(jax.random.fold_in(key, 4), (N_GX, N_GY, TD), 1, B * B + 1)
    return jnp.where(slot < counts[:, :, None], amounts, 0).reshape(-1).astype(jnp.int32)


def draw_tile_row(key, part):
    extent = N_GY * VBD
    device = jnp.arange(NT, dtype=jnp.int32) // TD
    outer = device // N_GY
    local = skewed_index(jax.random.fold_in(key, 21), (NT,), extent)
    return (outer * extent + local).astype(jnp.int32)


def draw_tile_col(key, part):
    extent = N_GX * VBD
    device = jnp.arange(NT, dtype=jnp.int32) // TD
    inner = device % N_GY
    local = skewed_index(jax.random.fold_in(key, 31), (NT,), extent)
    return ((local // VBD * N_GY + inner) * VBD + local % VBD).astype(jnp.int32)


def block_scale(key, dims, shards, smallest, high):
    level, own = 1.0, jax.random.fold_in(key, 6)
    for axis_at, blocks in shards:
        draws = jnp.exp(jax.random.uniform(jax.random.fold_in(own, axis_at), (blocks,), jnp.float32, smallest / len(shards), high / len(shards)))
        level = level * jnp.repeat(draws, dims[axis_at] // blocks).reshape([-1 if axis == axis_at else 1 for axis in range(len(dims))])
    return level


def gaussian(key, dims, scale, limit, shards=(), kind=jnp.bfloat16):
    loudness = block_scale(key, dims, shards, -0.22, 0.18) if shards else 1.0
    entries = jax.random.normal(key, dims, jnp.float32) * scale * loudness
    return jnp.minimum(jnp.maximum(entries, -limit), limit).astype(kind)


def setup_inputs(seed: int = 0) -> dict:
    key_of = jax.random.split(jax.random.key(seed), 6)
    features = gaussian(key_of[0], (NV, K), 1.0, 6.0, ((0, 32),))
    tile_vals = gaussian(key_of[1], (NT, B, B), (B * OWN // VBD) ** -0.5, 0.125, ((0, 32),))
    tile_row = draw_tile_row(jax.random.fold_in(key_of[5], 71), 0)
    tile_col = draw_tile_col(jax.random.fold_in(key_of[5], 71), 0)
    tile_work = draw_tile_work(jax.random.fold_in(key_of[5], 71), 0)
    return dict(features=features, tile_vals=tile_vals, tile_row=tile_row, tile_col=tile_col, tile_work=tile_work)


def reference(features, tile_vals, tile_row, tile_col, tile_work):
    devices = N_GX * N_GY
    live = (tile_work > 0).astype(jnp.int32).reshape(N_GX, N_GY, TD)
    counts = jnp.sum(live, axis=2)
    offsets = jnp.cumsum(counts, axis=1) - counts
    position = offsets[:, :, None] + jnp.arange(TD, dtype=jnp.int32)[None, None, :]
    row_index = jnp.arange(N_GX, dtype=jnp.int32)[:, None, None]
    target = (row_index * N_GY + position % N_GY) * OWN + position // N_GY
    target = jnp.where(live > 0, target, devices * OWN).reshape(-1).astype(jnp.int32)
    moved_vals = jnp.zeros((devices * OWN, B, B), jnp.bfloat16).at[target].set(tile_vals, mode="drop")
    moved_row = jnp.zeros((devices * OWN,), jnp.int32).at[target].set(tile_row, mode="drop")
    moved_col = jnp.zeros((devices * OWN,), jnp.int32).at[target].set(tile_col, mode="drop")
    moved_work = jnp.zeros((devices * OWN,), jnp.int32).at[target].set(tile_work, mode="drop")
    pattern = jnp.arange(B * B, dtype=jnp.int32).reshape(B, B)
    blocks = features.reshape(NB, B, K)

    def one_device(total, device):
        begin = (device * TD).astype(jnp.int32)
        values = lax.dynamic_slice_in_dim(tile_vals, begin, TD, 0)
        work = lax.dynamic_slice_in_dim(tile_work, begin, TD, 0)
        rows = lax.dynamic_slice_in_dim(tile_row, begin, TD, 0)
        columns = lax.dynamic_slice_in_dim(tile_col, begin, TD, 0)
        masked = jnp.where(pattern[None, :, :] < work[:, None, None], values, jnp.zeros((), jnp.bfloat16))
        vectors = jnp.take(blocks, columns, axis=0)
        products = jnp.einsum("tij,tjk->tik", masked.astype(jnp.float32), vectors.astype(jnp.float32))
        return total + jax.ops.segment_sum(products, rows, num_segments=NB), None

    summed, unused = lax.scan(one_device, jnp.zeros((NB, B, K), jnp.float32), jnp.arange(devices, dtype=jnp.int32))
    return summed.reshape(NB * B, K), moved_vals, moved_row, moved_col, moved_work
```

```python
import functools

import jax
import jax.numpy as jnp
from jax import lax
from jax.experimental import pallas as pl
from jax.experimental.pallas import tpu as pltpu
from jax.sharding import PartitionSpec as P

MESH = pl.DeviceIdType.MESH
FIRST, SECOND = 4, 2


def exchange(
    nx, ny, slots, vblocks, owned,
    work_in, row_in, col_in, feat_in, vals_ref,
    prod_ref, recv, table_ref,
    vbuf, stage, fbuf, mbuf, links, slinks, prefix, psend, precv, asend, arecv, qsend, qrecv, ssend, srecv,
    swork_ref, scol_ref, work_ref, row_ref, col_ref, feat_ref,
    lsem, isem, insem, ms, mr, fs, fr, ts, tr, ps, pr, xs, xr, qs, qr,
):
    share = slots // ny
    half = ny // 2
    nh = ny // 2
    near_heights = nh // 2
    order = feat_in.shape[1]
    gx, gy = lax.axis_index("gx"), lax.axis_index("gy")
    side, height = lax.rem(gy, 2), gy // 2
    upper, place_in_half = gy // half, lax.rem(gy, half)
    base = upper * half
    mate = lax.rem(gy + half, ny)

    load = pltpu.make_async_copy(vals_ref, vbuf, lsem)
    fetches = [
        pltpu.make_async_copy(src, dst, insem.at[i])
        for i, (src, dst) in enumerate((
            (work_in, work_ref), (row_in, row_ref), (col_in, col_ref), (feat_in, feat_ref),
            (work_in, swork_ref), (col_in, scol_ref),
        ))
    ]
    for copy in fetches:
        copy.start()
    load.start()

    def near(d):
        return base + lax.rem(place_in_half + d, half)

    def far(d):
        return half - base + lax.rem(place_in_half + d, half)

    def along_x(d):
        return (lax.rem(gx + d, nx), gy)

    barrier = pltpu.get_barrier_semaphore()
    for d in range(1, half):
        pl.semaphore_signal(barrier, inc=1, device_id=(gx, near(d)), device_id_type=MESH)
    pl.semaphore_signal(barrier, inc=1, device_id=(gx, mate), device_id_type=MESH)
    for d in range(1, nx):
        pl.semaphore_signal(barrier, inc=1, device_id=along_x(d), device_id_type=MESH)
    mbuf[gy] = jnp.zeros((8, 128), jnp.int32)
    for copy in fetches:
        copy.wait()
    for i, ref in enumerate((work_ref, row_ref, col_ref)):
        mbuf[gy, i : i + 1, 0:slots] = ref[...].reshape(1, slots)
    fbuf[pl.ds(0, vblocks)] = feat_ref[...]
    recv[slots] = jnp.zeros(recv.shape[1:], recv.dtype)

    pl.semaphore_wait(barrier, half - 1 + 1 + nx - 1)

    def remote(src, dst, send, arrive, where):
        return pltpu.make_async_remote_copy(
            src_ref=src, dst_ref=dst, send_sem=send, recv_sem=arrive,
            device_id=where, device_id_type=MESH,
        )

    near_metas = [
        remote(mbuf.at[gy], mbuf.at[gy], ms.at[d], mr.at[d], (gx, near(d))) for d in range(1, half)
    ]
    for copy in near_metas:
        copy.start()
    feats = [
        remote(feat_ref, fbuf.at[pl.ds(d * vblocks, vblocks)], fs.at[d], fr.at[d], along_x(d))
        for d in range(1, nx)
    ]
    for copy in feats:
        copy.start()
    for copy in near_metas:
        copy.wait_recv()
    far_metas = [
        remote(mbuf.at[gy], mbuf.at[gy], ms.at[half + d], mr.at[half + d], (gx, far(d)))
        for d in range(half)
    ]
    for copy in far_metas:
        copy.start()

    ahead, rest = jnp.int32(0), jnp.int32(0)
    for c in range(half):
        live = jnp.sum((mbuf[base + c, 0:1, :] > 0).astype(jnp.int32))
        ahead = ahead + jnp.where(c < place_in_half, live, 0)
        rest = rest + jnp.where(c < place_in_half, 0, live)
    start = lax.rem(jnp.where(upper > 0, ny * owned - rest, ahead), ny)

    load.wait()
    tiles = []

    def send_tiles(d):
        shift = lax.rem(gy + d + ny - start, ny)
        for k in range(share):
            stage[d * share + k] = vbuf[k * ny + shift]
        copy = remote(
            stage.at[pl.ds(d * share, share)], recv.at[pl.ds(gy * share, share)],
            ts.at[d], tr.at[d], (gx, lax.rem(gy + d, ny)),
        )
        copy.start()
        tiles.append(copy)

    cuts = (1 + FIRST * (ny - 1) // 7, 1 + (FIRST + SECOND) * (ny - 1) // 7)
    for d in range(1, cuts[0]):
        send_tiles(d)
    shift = lax.rem(gy + ny - start, ny)
    for k in range(share):
        recv[gy * share + k] = vbuf[k * ny + shift]

    prefix[slots] = jnp.zeros(prefix.shape[1:], jnp.float32)
    down = lax.broadcasted_iota(jnp.int32, (128, 128), 0)
    across = lax.broadcasted_iota(jnp.int32, (128, 128), 1)
    rows = jnp.where(across < slots, mbuf[gy, 1:2, :] - gx * (ny * vblocks), -1)
    upright = jnp.sum(jnp.where(down == across, rows, 0), axis=1, keepdims=True)
    prev = jnp.max(
        jnp.where((upright == rows) & (down < across), down, -1), axis=0, keepdims=True
    )
    last = jnp.max(jnp.where(upright == across, down, -1), axis=0, keepdims=True)
    links[...] = jnp.zeros((8, 128), jnp.int32)
    links[0:1, :] = jnp.where(prev < 0, slots, prev)
    links[1:2, :] = jnp.where(last < 0, slots, last)
    listing = pltpu.make_async_copy(links, slinks, isem)
    listing.start()
    listing.wait()
    for copy in feats:
        copy.wait_recv()
    pattern = lax.broadcasted_iota(jnp.int32, (order, order), 0) * order + lax.broadcasted_iota(
        jnp.int32, (order, order), 1
    )
    group = 4

    def multiply(step, carry):
        terms = []
        for u in range(group):
            t = step * group + u
            values = vbuf[t].astype(jnp.float32)
            masked = jnp.where(pattern < swork_ref[t], values, 0.0).astype(jnp.bfloat16)
            col = scol_ref[t]
            back = lax.rem(gx - col // vblocks // ny + nx, nx)
            block = fbuf[back * vblocks + lax.rem(col, vblocks)]
            terms.append(jnp.dot(masked, block, preferred_element_type=jnp.float32))
        for u in range(group):
            t = step * group + u
            prefix[t] = terms[u] + prefix[slinks[0, t]]
        return carry

    lax.fori_loop(0, slots // group, multiply, 0)

    def summed(h, q, v):
        return prefix[slinks[1, (h * 2 + q) * vblocks + v]]

    def beside(u):
        return upper * near_heights + lax.rem(lax.rem(height, near_heights) + u, near_heights)

    def heights(u):
        h = beside(u)
        return (h, nh - 1 - h)

    span = 2 * vblocks
    halves = {}
    for u in [*range(1, near_heights), 0]:
        for w, h in enumerate(heights(u)):
            for v in range(vblocks):
                psend[u * span + w * vblocks + v] = summed(h, 1 - side, v)
        where = pl.ds(u * span, span)
        copy = remote(
            psend.at[where], precv.at[where], ps.at[u], pr.at[u], (gx, gy + 1 - 2 * side)
        )
        copy.start()
        halves[u] = copy
    for d in range(cuts[0], cuts[1]):
        send_tiles(d)

    joins = []
    for u in range(1, near_heights):
        halves[u].wait_recv()
        for w, h in enumerate(heights(u)):
            for v in range(vblocks):
                at = u * span + w * vblocks + v
                asend[at] = summed(h, side, v) + precv[at]
        where = pl.ds(u * span, span)
        copy = remote(
            asend.at[where], arecv.at[where], xs.at[u], xr.at[u], (gx, beside(u) * 2 + side)
        )
        copy.start()
        joins.append(copy)
    for d in range(cuts[1], ny):
        send_tiles(d)

    halves[0].wait_recv()
    for copy in joins:
        copy.wait_recv()

    def gathered(w, h, v):
        total = summed(h, side, v) + precv[w * vblocks + v]
        for u in range(1, near_heights):
            total = total + arecv[u * span + w * vblocks + v]
        return total

    mirror = nh - 1 - height
    ssend[...] = jnp.zeros(ssend.shape, jnp.float32)
    for v in range(vblocks):
        term = gathered(1, mirror, v)
        peak = jnp.max(jnp.abs(term), axis=0, keepdims=True)
        small = peak < 2.0**-62
        term, peak = term * jnp.where(small, 2.0**64, 1.0), peak * jnp.where(small, 2.0**64, 1.0)
        term = term * jnp.where(peak > 0, 32767.0 / jnp.where(peak > 0, peak, 1.0), 0.0)
        term = (term + jnp.where(term < 0, -0.5, 0.5)).astype(jnp.int32)
        qsend[v] = term.astype(jnp.int16)
        ssend[v : v + 1, :] = peak * (1.0 / 32767.0)
        ssend[vblocks + v : vblocks + v + 1, :] = jnp.where(small, 2.0**-64, 1.0)
    owner = (gx, mirror * 2 + side)
    partials = [
        remote(ssend, srecv, qs.at[0], qr.at[0], owner),
        remote(qsend, qrecv, qs.at[1], qr.at[1], owner),
    ]
    for copy in partials:
        copy.start()

    for copy in far_metas:
        copy.wait_recv()
    count = [jnp.sum((mbuf[c, 0:1, :] > 0).astype(jnp.int32)) for c in range(ny)]
    first = [jnp.int32(0)]
    for c in range(ny - 1):
        first.append(first[-1] + count[c])
    table_ref[...] = jnp.zeros(table_ref.shape, jnp.int32)
    slot = lax.broadcasted_iota(jnp.int32, (1, 128), 1)
    wanted = slot * ny + gy
    at = jnp.full((1, 128), slots, jnp.int32)
    for c in range(ny):
        offset = c * share + (gy - first[c] + slots * ny) // ny - slots
        here = (wanted >= first[c]) & (wanted < first[c] + count[c])
        at = jnp.where(here, slot + offset, at)
    table_ref[3:4, :] = at
    lane = lax.broadcasted_iota(jnp.int32, (owned, 128), 1)
    line = lax.broadcasted_iota(jnp.int32, (owned, 128), 0)
    wanted = line * ny + gy
    sums = [jnp.zeros((owned, 128), jnp.int32) for _ in range(3)]
    for c in range(ny):
        work = mbuf[c, 0:1, :]
        hit = (lane + first[c] == wanted) & (work > 0)
        for i in range(3):
            sums[i] = sums[i] + jnp.where(hit, mbuf[c, i : i + 1, :], 0)
    for i in range(3):
        column = jnp.sum(sums[i], axis=1, keepdims=True)
        spread = jnp.where(line == lane, jnp.broadcast_to(column, (owned, 128)), 0)
        table_ref[i : i + 1, :] = jnp.sum(spread, axis=0, keepdims=True)

    own = [gathered(0, height, v) for v in range(vblocks)]
    for copy in partials:
        copy.wait_recv()
    for v in range(vblocks):
        coded = qrecv[v].astype(jnp.int32).astype(jnp.float32)
        scale = srecv[v : v + 1, :]
        prod_ref[v] = own[v] + coded * scale * srecv[vblocks + v : vblocks + v + 1, :]
    for copy in tiles:
        copy.wait_recv()
    for copy in (*near_metas, *far_metas, *feats, *tiles, *halves.values(), *joins, *partials):
        copy.wait_send()


def deliver(owned, table, meta_ref, prod_ref, recv, prod_out, moved_out, row_out, col_out, work_out, sems, psem):
    copies = [
        pltpu.make_async_copy(recv.at[table[3, s]], moved_out.at[s], sems.at[s]) for s in range(owned)
    ]
    for copy in copies:
        copy.start()
    product = pltpu.make_async_copy(prod_ref, prod_out, psem)
    product.start()
    for i, ref in enumerate((work_out, row_out, col_out)):
        ref[...] = meta_ref[i, 0:owned]
    for copy in copies:
        copy.wait()
    product.wait()


def size(shape, kind):
    total = jnp.dtype(kind).itemsize
    for extent in shape:
        total *= extent
    return total


def on_device(nx, ny, features, tile_vals, tile_row, tile_col, tile_work):
    slots, order = tile_vals.shape[:2]
    width = features.shape[1]
    vblocks = features.shape[0] // order
    owned = slots // 2
    near_heights = ny // 4
    half_blocks = near_heights * 2 * vblocks
    vmem = pl.BlockSpec(memory_space=pltpu.VMEM)
    smem = pl.BlockSpec(memory_space=pltpu.SMEM)
    anywhere = pl.BlockSpec(memory_space=pl.ANY)
    hbm = pl.BlockSpec(memory_space=pltpu.HBM)
    bf, f32, i32 = jnp.bfloat16, jnp.float32, jnp.int32
    dma = pltpu.SemaphoreType.DMA
    buffers = [
        ((slots, order, order), bf),
        ((slots, order, order), bf),
        ((nx * vblocks, order, width), bf),
        ((ny, 8, 128), i32),
        ((8, 128), i32),
        None,
        ((slots + 1, order, width), f32),
        ((half_blocks, order, width), f32),
        ((half_blocks, order, width), f32),
        ((half_blocks, order, width), f32),
        ((half_blocks, order, width), f32),
        ((vblocks, order, width), jnp.int16),
        ((vblocks, order, width), jnp.int16),
        ((8, width), f32),
        ((8, width), f32),
    ]
    results = (
        jax.ShapeDtypeStruct((vblocks, order, width), f32),
        jax.ShapeDtypeStruct((slots + 1, order, order), bf),
        jax.ShapeDtypeStruct((8, 128), i32),
    )
    need = sum(size(*b) for b in buffers if b) + sum(size(r.shape, r.dtype) for r in results)
    product, recv, table = pl.pallas_call(
        functools.partial(exchange, nx, ny, slots, vblocks, owned),
        out_shape=results,
        in_specs=[hbm] * 5,
        out_specs=(vmem, vmem, vmem),
        scratch_shapes=[
            pltpu.VMEM(*b) if b else pltpu.SMEM((8, 128), i32) for b in buffers
        ] + [
            pltpu.SMEM((slots,), i32),
            pltpu.SMEM((slots,), i32),
            pltpu.VMEM((slots,), i32),
            pltpu.VMEM((slots,), i32),
            pltpu.VMEM((slots,), i32),
            pltpu.VMEM((vblocks, order, width), bf),
            dma, dma, dma((6,)), dma((ny,)), dma((ny,)), dma((nx,)), dma((nx,)),
            dma((ny,)), dma((ny,)), dma((near_heights,)), dma((near_heights,)),
            dma((near_heights,)), dma((near_heights,)), dma((2,)), dma((2,)),
        ],
        compiler_params=pltpu.CompilerParams(
            collective_id=0, has_side_effects=True, vmem_limit_bytes=need + 4 * 2**20
        ),
    )(
        tile_work, tile_row, tile_col,
        features.reshape(vblocks, order, width), tile_vals,
    )
    index = jax.ShapeDtypeStruct((owned,), i32)
    product, moved, row, col, work = pl.pallas_call(
        functools.partial(deliver, owned),
        out_shape=(
            jax.ShapeDtypeStruct((vblocks, order, width), f32),
            jax.ShapeDtypeStruct((owned, order, order), bf),
            index, index, index,
        ),
        in_specs=[smem, vmem, vmem, vmem],
        out_specs=(hbm, hbm, vmem, vmem, vmem),
        scratch_shapes=[dma((owned,)), dma],
        compiler_params=pltpu.CompilerParams(vmem_limit_bytes=4 * 2**20),
    )(table, table, product, recv)
    return product.reshape(vblocks * order, width), moved, row, col, work


def solution(mesh):
    both = ("gx", "gy")
    return jax.shard_map(
        functools.partial(on_device, mesh.shape["gx"], mesh.shape["gy"]),
        mesh=mesh,
        in_specs=(P(both, None), P(both, None, None), P(both), P(both), P(both)),
        out_specs=(P(both, None), P(both, None, None), P(both), P(both), P(both)),
        check_vma=False,
    )
```

```python
import functools

import jax
import jax.numpy as jnp
from jax import lax
from jax.experimental import pallas as pl
from jax.experimental.pallas import tpu as pltpu
from jax.sharding import PartitionSpec as P

MESH = pl.DeviceIdType.MESH


def exchange(
    nx, ny, slots, vblocks, owned,
    work_in, row_in, col_in, feat_in, vals_ref,
    prod_ref, recv, table_ref,
    vbuf, stage, fbuf, mbuf, links, slinks, prefix, psend, precv, asend, arecv, qsend, qrecv, ssend, srecv,
    swork_ref, scol_ref, work_ref, row_ref, col_ref, feat_ref,
    lsem, isem, insem, ms, mr, fs, fr, ts, tr, ps, pr, xs, xr, qs, qr,
):
    share = slots // ny
    half = ny // 2
    nh = ny // 2
    near_heights = nh // 2
    order = feat_in.shape[1]
    gx, gy = lax.axis_index("gx"), lax.axis_index("gy")
    side, height = lax.rem(gy, 2), gy // 2
    upper, place_in_half = gy // half, lax.rem(gy, half)
    base = upper * half
    mate = lax.rem(gy + half, ny)

    load = pltpu.make_async_copy(vals_ref, vbuf, lsem)
    fetches = [
        pltpu.make_async_copy(src, dst, insem.at[i])
        for i, (src, dst) in enumerate((
            (work_in, work_ref), (row_in, row_ref), (col_in, col_ref), (feat_in, feat_ref),
            (work_in, swork_ref), (col_in, scol_ref),
        ))
    ]
    for copy in fetches:
        copy.start()
    load.start()

    def near(d):
        return base + lax.rem(place_in_half + d, half)

    def far(d):
        return half - base + lax.rem(place_in_half + d, half)

    def along_x(d):
        return (lax.rem(gx + d, nx), gy)

    barrier = pltpu.get_barrier_semaphore()
    for d in range(1, half):
        pl.semaphore_signal(barrier, inc=1, device_id=(gx, near(d)), device_id_type=MESH)
    pl.semaphore_signal(barrier, inc=1, device_id=(gx, mate), device_id_type=MESH)
    for d in range(1, nx):
        pl.semaphore_signal(barrier, inc=1, device_id=along_x(d), device_id_type=MESH)
    mbuf[gy] = jnp.zeros((8, 128), jnp.int32)
    for copy in fetches:
        copy.wait()
    for i, ref in enumerate((work_ref, row_ref, col_ref)):
        mbuf[gy, i : i + 1, 0:slots] = ref[...].reshape(1, slots)
    fbuf[pl.ds(0, vblocks)] = feat_ref[...]
    recv[slots] = jnp.zeros(recv.shape[1:], recv.dtype)

    pl.semaphore_wait(barrier, half - 1 + 1 + nx - 1)

    def remote(src, dst, send, arrive, where):
        return pltpu.make_async_remote_copy(
            src_ref=src, dst_ref=dst, send_sem=send, recv_sem=arrive,
            device_id=where, device_id_type=MESH,
        )

    near_metas = [
        remote(mbuf.at[gy], mbuf.at[gy], ms.at[d], mr.at[d], (gx, near(d))) for d in range(1, half)
    ]
    for copy in near_metas:
        copy.start()
    feats = [
        remote(feat_ref, fbuf.at[pl.ds(d * vblocks, vblocks)], fs.at[d], fr.at[d], along_x(d))
        for d in range(1, nx)
    ]
    for copy in feats:
        copy.start()
    for copy in near_metas:
        copy.wait_recv()
    far_metas = [
        remote(mbuf.at[gy], mbuf.at[gy], ms.at[half + d], mr.at[half + d], (gx, far(d)))
        for d in range(half)
    ]
    for copy in far_metas:
        copy.start()

    ahead, rest = jnp.int32(0), jnp.int32(0)
    for c in range(half):
        live = jnp.sum((mbuf[base + c, 0:1, :] > 0).astype(jnp.int32))
        ahead = ahead + jnp.where(c < place_in_half, live, 0)
        rest = rest + jnp.where(c < place_in_half, 0, live)
    start = lax.rem(jnp.where(upper > 0, ny * owned - rest, ahead), ny)

    load.wait()
    tiles = []

    def send_tiles(across, up, over):
        h = (1 - upper if across else upper) * near_heights + lax.rem(
            lax.rem(height, near_heights) + up, near_heights
        )
        e = h * 2 + (1 - side if over else side)
        i = (across * near_heights + up) * 2 + over
        shift = lax.rem(e + ny - start, ny)
        for k in range(share):
            stage[i * share + k] = vbuf[k * ny + shift]
        copy = remote(
            stage.at[pl.ds(i * share, share)], recv.at[pl.ds(gy * share, share)],
            ts.at[i], tr.at[i], (gx, e),
        )
        copy.start()
        tiles.append(copy)

    near_line = [(0, u, 0) for u in range(1, near_heights)]
    near_cross = [(0, u, 1) for u in range(1, near_heights)]
    far_line = [(1, u, 0) for u in range(near_heights)]
    far_cross = [(1, u, 1) for u in range(near_heights)]
    pair = [(0, 0, 1)]
    middle = near_heights // 2
    batches = [near_line + far_line + pair, far_cross[:middle], [], far_cross[middle:] + near_cross]
    for way in batches[0]:
        send_tiles(*way)
    shift = lax.rem(gy + ny - start, ny)
    for k in range(share):
        recv[gy * share + k] = vbuf[k * ny + shift]

    prefix[slots] = jnp.zeros(prefix.shape[1:], jnp.float32)
    down = lax.broadcasted_iota(jnp.int32, (128, 128), 0)
    across = lax.broadcasted_iota(jnp.int32, (128, 128), 1)
    rows = jnp.where(across < slots, mbuf[gy, 1:2, :] - gx * (ny * vblocks), -1)
    upright = jnp.sum(jnp.where(down == across, rows, 0), axis=1, keepdims=True)
    prev = jnp.max(
        jnp.where((upright == rows) & (down < across), down, -1), axis=0, keepdims=True
    )
    last = jnp.max(jnp.where(upright == across, down, -1), axis=0, keepdims=True)
    links[...] = jnp.zeros((8, 128), jnp.int32)
    links[0:1, :] = jnp.where(prev < 0, slots, prev)
    links[1:2, :] = jnp.where(last < 0, slots, last)
    listing = pltpu.make_async_copy(links, slinks, isem)
    listing.start()
    listing.wait()
    for copy in feats:
        copy.wait_recv()
    pattern = lax.broadcasted_iota(jnp.int32, (order, order), 0) * order + lax.broadcasted_iota(
        jnp.int32, (order, order), 1
    )
    group = 4

    def multiply(step, carry):
        terms = []
        for u in range(group):
            t = step * group + u
            values = vbuf[t].astype(jnp.float32)
            masked = jnp.where(pattern < swork_ref[t], values, 0.0).astype(jnp.bfloat16)
            col = scol_ref[t]
            back = lax.rem(gx - col // vblocks // ny + nx, nx)
            block = fbuf[back * vblocks + lax.rem(col, vblocks)]
            terms.append(jnp.dot(masked, block, preferred_element_type=jnp.float32))
        for u in range(group):
            t = step * group + u
            prefix[t] = terms[u] + prefix[slinks[0, t]]
        return carry

    lax.fori_loop(0, slots // group, multiply, 0)

    def summed(h, q, v):
        return prefix[slinks[1, (h * 2 + q) * vblocks + v]]

    def beside(u):
        return upper * near_heights + lax.rem(lax.rem(height, near_heights) + u, near_heights)

    def heights(u):
        h = beside(u)
        return (h, nh - 1 - h)

    span = 2 * vblocks
    halves = {}
    for u in [*range(1, near_heights), 0]:
        for w, h in enumerate(heights(u)):
            for v in range(vblocks):
                psend[u * span + w * vblocks + v] = summed(h, 1 - side, v)
        where = pl.ds(u * span, span)
        copy = remote(
            psend.at[where], precv.at[where], ps.at[u], pr.at[u], (gx, gy + 1 - 2 * side)
        )
        copy.start()
        halves[u] = copy
    for way in batches[1]:
        send_tiles(*way)

    joins = []
    for u in range(1, near_heights):
        halves[u].wait_recv()
        for w, h in enumerate(heights(u)):
            for v in range(vblocks):
                at = u * span + w * vblocks + v
                asend[at] = summed(h, side, v) + precv[at]
        where = pl.ds(u * span, span)
        copy = remote(
            asend.at[where], arecv.at[where], xs.at[u], xr.at[u], (gx, beside(u) * 2 + side)
        )
        copy.start()
        joins.append(copy)
    for way in batches[2]:
        send_tiles(*way)

    halves[0].wait_recv()
    for copy in joins:
        copy.wait_recv()

    def gathered(w, h, v):
        total = summed(h, side, v) + precv[w * vblocks + v]
        for u in range(1, near_heights):
            total = total + arecv[u * span + w * vblocks + v]
        return total

    mirror = nh - 1 - height
    ssend[...] = jnp.zeros(ssend.shape, jnp.float32)
    for v in range(vblocks):
        term = gathered(1, mirror, v)
        peak = jnp.max(jnp.abs(term), axis=0, keepdims=True)
        small = peak < 2.0**-62
        term, peak = term * jnp.where(small, 2.0**64, 1.0), peak * jnp.where(small, 2.0**64, 1.0)
        term = term * jnp.where(peak > 0, 32767.0 / jnp.where(peak > 0, peak, 1.0), 0.0)
        term = (term + jnp.where(term < 0, -0.5, 0.5)).astype(jnp.int32)
        qsend[v] = term.astype(jnp.int16)
        ssend[v : v + 1, :] = peak * (1.0 / 32767.0)
        ssend[vblocks + v : vblocks + v + 1, :] = jnp.where(small, 2.0**-64, 1.0)
    owner = (gx, mirror * 2 + side)
    partials = [
        remote(ssend, srecv, qs.at[0], qr.at[0], owner),
        remote(qsend, qrecv, qs.at[1], qr.at[1], owner),
    ]
    for copy in partials:
        copy.start()
    for way in batches[3]:
        send_tiles(*way)

    for copy in far_metas:
        copy.wait_recv()
    count = [jnp.sum((mbuf[c, 0:1, :] > 0).astype(jnp.int32)) for c in range(ny)]
    first = [jnp.int32(0)]
    for c in range(ny - 1):
        first.append(first[-1] + count[c])
    table_ref[...] = jnp.zeros(table_ref.shape, jnp.int32)
    slot = lax.broadcasted_iota(jnp.int32, (1, 128), 1)
    wanted = slot * ny + gy
    at = jnp.full((1, 128), slots, jnp.int32)
    for c in range(ny):
        offset = c * share + (gy - first[c] + slots * ny) // ny - slots
        here = (wanted >= first[c]) & (wanted < first[c] + count[c])
        at = jnp.where(here, slot + offset, at)
    table_ref[3:4, :] = at
    lane = lax.broadcasted_iota(jnp.int32, (owned, 128), 1)
    line = lax.broadcasted_iota(jnp.int32, (owned, 128), 0)
    wanted = line * ny + gy
    sums = [jnp.zeros((owned, 128), jnp.int32) for _ in range(3)]
    for c in range(ny):
        work = mbuf[c, 0:1, :]
        hit = (lane + first[c] == wanted) & (work > 0)
        for i in range(3):
            sums[i] = sums[i] + jnp.where(hit, mbuf[c, i : i + 1, :], 0)
    for i in range(3):
        column = jnp.sum(sums[i], axis=1, keepdims=True)
        spread = jnp.where(line == lane, jnp.broadcast_to(column, (owned, 128)), 0)
        table_ref[i : i + 1, :] = jnp.sum(spread, axis=0, keepdims=True)

    own = [gathered(0, height, v) for v in range(vblocks)]
    for copy in partials:
        copy.wait_recv()
    for v in range(vblocks):
        coded = qrecv[v].astype(jnp.int32).astype(jnp.float32)
        scale = srecv[v : v + 1, :]
        prod_ref[v] = own[v] + coded * scale * srecv[vblocks + v : vblocks + v + 1, :]
    for copy in tiles:
        copy.wait_recv()
    for copy in (*near_metas, *far_metas, *feats, *tiles, *halves.values(), *joins, *partials):
        copy.wait_send()


def deliver(owned, table, meta_ref, prod_ref, recv, prod_out, moved_out, row_out, col_out, work_out, sems, psem):
    copies = [
        pltpu.make_async_copy(recv.at[table[3, s]], moved_out.at[s], sems.at[s]) for s in range(owned)
    ]
    for copy in copies:
        copy.start()
    product = pltpu.make_async_copy(prod_ref, prod_out, psem)
    product.start()
    for i, ref in enumerate((work_out, row_out, col_out)):
        ref[...] = meta_ref[i, 0:owned]
    for copy in copies:
        copy.wait()
    product.wait()


def size(shape, kind):
    total = jnp.dtype(kind).itemsize
    for extent in shape:
        total *= extent
    return total


def on_device(nx, ny, features, tile_vals, tile_row, tile_col, tile_work):
    slots, order = tile_vals.shape[:2]
    width = features.shape[1]
    vblocks = features.shape[0] // order
    owned = slots // 2
    near_heights = ny // 4
    half_blocks = near_heights * 2 * vblocks
    vmem = pl.BlockSpec(memory_space=pltpu.VMEM)
    smem = pl.BlockSpec(memory_space=pltpu.SMEM)
    anywhere = pl.BlockSpec(memory_space=pl.ANY)
    hbm = pl.BlockSpec(memory_space=pltpu.HBM)
    bf, f32, i32 = jnp.bfloat16, jnp.float32, jnp.int32
    dma = pltpu.SemaphoreType.DMA
    buffers = [
        ((slots, order, order), bf),
        ((slots, order, order), bf),
        ((nx * vblocks, order, width), bf),
        ((ny, 8, 128), i32),
        ((8, 128), i32),
        None,
        ((slots + 1, order, width), f32),
        ((half_blocks, order, width), f32),
        ((half_blocks, order, width), f32),
        ((half_blocks, order, width), f32),
        ((half_blocks, order, width), f32),
        ((vblocks, order, width), jnp.int16),
        ((vblocks, order, width), jnp.int16),
        ((8, width), f32),
        ((8, width), f32),
    ]
    results = (
        jax.ShapeDtypeStruct((vblocks, order, width), f32),
        jax.ShapeDtypeStruct((slots + 1, order, order), bf),
        jax.ShapeDtypeStruct((8, 128), i32),
    )
    need = sum(size(*b) for b in buffers if b) + sum(size(r.shape, r.dtype) for r in results)
    product, recv, table = pl.pallas_call(
        functools.partial(exchange, nx, ny, slots, vblocks, owned),
        out_shape=results,
        in_specs=[hbm] * 5,
        out_specs=(vmem, vmem, vmem),
        scratch_shapes=[
            pltpu.VMEM(*b) if b else pltpu.SMEM((8, 128), i32) for b in buffers
        ] + [
            pltpu.SMEM((slots,), i32),
            pltpu.SMEM((slots,), i32),
            pltpu.VMEM((slots,), i32),
            pltpu.VMEM((slots,), i32),
            pltpu.VMEM((slots,), i32),
            pltpu.VMEM((vblocks, order, width), bf),
            dma, dma, dma((6,)), dma((ny,)), dma((ny,)), dma((nx,)), dma((nx,)),
            dma((ny,)), dma((ny,)), dma((near_heights,)), dma((near_heights,)),
            dma((near_heights,)), dma((near_heights,)), dma((2,)), dma((2,)),
        ],
        compiler_params=pltpu.CompilerParams(
            collective_id=0, has_side_effects=True, vmem_limit_bytes=need + 4 * 2**20
        ),
    )(*(
        pltpu.with_memory_space_constraint(x, pltpu.HBM)
        for x in (
            tile_work, tile_row, tile_col,
            features.reshape(vblocks, order, width), tile_vals,
        )
    ))
    index = jax.ShapeDtypeStruct((owned,), i32)
    product, moved, row, col, work = pl.pallas_call(
        functools.partial(deliver, owned),
        out_shape=(
            jax.ShapeDtypeStruct((vblocks, order, width), f32),
            jax.ShapeDtypeStruct((owned, order, order), bf),
            index, index, index,
        ),
        in_specs=[smem, vmem, vmem, vmem],
        out_specs=(hbm, hbm, vmem, vmem, vmem),
        scratch_shapes=[dma((owned,)), dma],
        compiler_params=pltpu.CompilerParams(vmem_limit_bytes=4 * 2**20),
    )(table, table, product, recv)
    return product.reshape(vblocks * order, width), moved, row, col, work


def solution(mesh):
    both = ("gx", "gy")
    return jax.shard_map(
        functools.partial(on_device, mesh.shape["gx"], mesh.shape["gy"]),
        mesh=mesh,
        in_specs=(P(both, None), P(both, None, None), P(both), P(both), P(both)),
        out_specs=(P(both, None), P(both, None, None), P(both), P(both), P(both)),
        check_vma=False,
    )
```

```python
import functools

import jax
import jax.numpy as jnp
from jax import lax
from jax.experimental import pallas as pl
from jax.experimental.pallas import tpu as pltpu
from jax.sharding import PartitionSpec as P

MESH = pl.DeviceIdType.MESH


def exchange(
    nx, ny, slots, vblocks, owned,
    work_in, row_in, col_in, feat_in, vals_ref,
    prod_ref, moved_ref, table_ref,
    vbuf, stage, recv, fbuf, mbuf, live_ref, links, slinks, prefix,
    psend, precv, asend, arecv, qsend, qrecv, ssend, srecv,
    swork_ref, scol_ref, work_ref, row_ref, col_ref, feat_ref, ready, xready,
    lsem, isem, insem, ms, mr, fs, fr, ts, tr, ps, pr, xs, xr, qs, qr,
):
    share = slots // ny
    half = ny // 2
    nh = ny // 2
    near_heights = nh // 2
    order = feat_in.shape[1]
    gx, gy = lax.axis_index("gx"), lax.axis_index("gy")
    side, height = lax.rem(gy, 2), gy // 2
    upper, place_in_half = gy // half, lax.rem(gy, half)
    base = upper * half

    load = pltpu.make_async_copy(vals_ref, vbuf, lsem)
    fetches = [
        pltpu.make_async_copy(src, dst, insem.at[i])
        for i, (src, dst) in enumerate((
            (work_in, work_ref), (row_in, row_ref), (col_in, col_ref), (feat_in, feat_ref),
            (work_in, swork_ref), (col_in, scol_ref),
        ))
    ]
    for copy in fetches:
        copy.start()
    load.start()

    def near(d):
        return base + lax.rem(place_in_half + d, half)

    def around(d):
        return lax.rem(gy + d, ny)

    def along_x(d):
        return lax.rem(gx + d, nx)

    def remote(src, dst, send, arrive, where):
        return pltpu.make_async_remote_copy(
            src_ref=src, dst_ref=dst, send_sem=send, recv_sem=arrive,
            device_id=where, device_id_type=MESH,
        )

    def landed(ref, sem):
        pltpu.make_async_copy(ref, ref, sem).wait()

    def signal(sem, where):
        pl.semaphore_signal(sem, inc=1, device_id=where, device_id_type=MESH)

    def rank(c):
        tie = jnp.where(c < half, half - 1 - c, c)
        return (c // 2 + lax.rem(c, 2)) * ny + tie

    mine = rank(gy)

    def above(e):
        return rank(e) > mine

    def below(e):
        return rank(e) < mine

    lower = gx
    for d in range(1, ny):
        lower = lower + jnp.where(below(around(d)), 1, 0)
    barrier = pltpu.get_barrier_semaphore()
    for d in range(1, ny):
        pl.when(above(around(d)))(functools.partial(signal, barrier, (gx, around(d))))
    for d in range(1, nx):
        pl.when(along_x(d) > gx)(functools.partial(signal, barrier, (along_x(d), gy)))
    mbuf[gy] = jnp.zeros(mbuf.shape[1:], jnp.int32)
    recv[slots] = jnp.zeros(recv.shape[1:], recv.dtype)
    pl.when(lower > 0)(lambda: pl.semaphore_wait(barrier, lower))
    for d in range(1, ny):
        pl.when(below(around(d)))(functools.partial(signal, ready.at[gy], (gx, around(d))))
    for d in range(1, nx):
        pl.when(along_x(d) < gx)(functools.partial(signal, xready.at[gx], (along_x(d), gy)))
    for copy in fetches:
        copy.wait()
    for i, ref in enumerate((work_ref, row_ref, col_ref)):
        mbuf[gy, i : i + 1, 0:slots] = ref[...].reshape(1, slots)

    def answered(e):
        pl.when(above(e))(lambda: pl.semaphore_wait(ready.at[e], 1))

    def meta(c, e, i):
        return remote(mbuf.at[c], mbuf.at[c], ms, mr.at[i], (gx, e))

    metas = [meta(gy, near(d), d) for d in range(1, half)]
    for d in range(1, half):
        pl.when(below(near(d)))(metas[d - 1].start)
    feats = [
        remote(
            feat_ref, fbuf.at[pl.ds(d * vblocks, vblocks)], fs, fr, (along_x(d), gy)
        )
        for d in range(1, nx)
    ]
    for d in range(1, nx):
        pl.when(along_x(d) < gx)(feats[d - 1].start)
    for d in range(1, half):
        answered(near(d))
        pl.when(above(near(d)))(metas[d - 1].start)
    for d in range(1, nx):
        pl.when(along_x(d) > gx)(lambda d=d: pl.semaphore_wait(xready.at[along_x(d)], 1))
        pl.when(along_x(d) > gx)(feats[d - 1].start)
    fbuf[pl.ds(0, vblocks)] = feat_ref[...]

    def needed(c):
        return jnp.where(upper > 0, c > gy, c < gy)

    def alive(c):
        return (mbuf[c, 0:1, :] > 0).astype(jnp.int32)

    live_ref[...] = alive(gy) * jnp.where(upper > 0, 1, 0)
    for d in range(1, half):
        @pl.when(needed(near(half - d)))
        def _(c=near(half - d), d=d):
            meta(c, c, d).wait_recv()
            live_ref[...] += alive(c)
    passed = jnp.sum(live_ref[...])
    start = lax.rem(jnp.where(upper > 0, ny * owned - passed, passed), ny)

    load.wait()
    tiles = []

    def target(across, up, over):
        h = (1 - upper if across else upper) * near_heights + lax.rem(
            lax.rem(height, near_heights) + up, near_heights
        )
        return h * 2 + (1 - side if over else side)

    def send_meta(across, up, over):
        e = target(across, up, over)
        answered(e)
        metas.append(meta(gy, e, 0))
        metas[-1].start()

    def send_tiles(across, up, over):
        e = target(across, up, over)
        i = (across * near_heights + up) * 2 + over
        shift = lax.rem(e + ny - start, ny)
        for k in range(share):
            stage[i * share + k] = vbuf[k * ny + shift]
        copy = remote(
            stage.at[pl.ds(i * share, share)], recv.at[pl.ds(gy * share, share)],
            ts, tr, (gx, e),
        )
        copy.start()
        tiles.append(copy)

    near_line = [(0, u, 0) for u in range(1, near_heights)]
    near_cross = [(0, u, 1) for u in range(1, near_heights)]
    far_line = [(1, u, 0) for u in range(near_heights)]
    far_cross = [(1, u, 1) for u in range(near_heights)]
    pair = [(0, 0, 1)]
    middle = near_heights // 2
    batches = [far_line[:middle] + near_line + pair + far_line[middle:], far_cross[:middle], near_cross, far_cross[middle:]]
    told = []
    for way in batches[0]:
        if way[0]:
            send_meta(*way)
            told.append(way)
        send_tiles(*way)
    shift = lax.rem(gy + ny - start, ny)
    for k in range(share):
        recv[gy * share + k] = vbuf[k * ny + shift]

    prefix[slots] = jnp.zeros(prefix.shape[1:], jnp.float32)
    down = lax.broadcasted_iota(jnp.int32, (128, 128), 0)
    across = lax.broadcasted_iota(jnp.int32, (128, 128), 1)
    rows = jnp.where(across < slots, mbuf[gy, 1:2, :] - gx * (ny * vblocks), -1)
    upright = jnp.sum(jnp.where(down == across, rows, 0), axis=1, keepdims=True)
    prev = jnp.max(
        jnp.where((upright == rows) & (down < across), down, -1), axis=0, keepdims=True
    )
    last = jnp.max(jnp.where(upright == across, down, -1), axis=0, keepdims=True)
    links[...] = jnp.zeros((8, 128), jnp.int32)
    links[0:1, :] = jnp.where(prev < 0, slots, prev)
    links[1:2, :] = jnp.where(last < 0, slots, last)
    listing = pltpu.make_async_copy(links, slinks, isem)
    listing.start()
    listing.wait()
    landed(fbuf.at[pl.ds(vblocks, (nx - 1) * vblocks)], fr)
    pattern = lax.broadcasted_iota(jnp.int32, (order, order), 0) * order + lax.broadcasted_iota(
        jnp.int32, (order, order), 1
    )
    group = 4

    def multiply(step, carry):
        terms = []
        for u in range(group):
            t = step * group + u
            values = vbuf[t].astype(jnp.float32)
            masked = jnp.where(pattern < swork_ref[t], values, 0.0).astype(jnp.bfloat16)
            col = scol_ref[t]
            back = lax.rem(gx - col // vblocks // ny + nx, nx)
            block = fbuf[back * vblocks + lax.rem(col, vblocks)]
            terms.append(jnp.dot(masked, block, preferred_element_type=jnp.float32))
        for u in range(group):
            t = step * group + u
            prefix[t] = terms[u] + prefix[slinks[0, t]]
        return carry

    lax.fori_loop(0, slots // group, multiply, 0)

    def summed(h, q, v):
        return prefix[slinks[1, (h * 2 + q) * vblocks + v]]

    def beside(u):
        return upper * near_heights + lax.rem(lax.rem(height, near_heights) + u, near_heights)

    def heights(u):
        h = beside(u)
        return (h, nh - 1 - h)

    span = 2 * vblocks
    halves = {}
    for u in [*range(1, near_heights), 0]:
        for w, h in enumerate(heights(u)):
            for v in range(vblocks):
                psend[u * span + w * vblocks + v] = summed(h, 1 - side, v)
        where = pl.ds(u * span, span)
        copy = remote(
            psend.at[where], precv.at[where], ps, pr.at[u], (gx, gy + 1 - 2 * side)
        )
        copy.start()
        halves[u] = copy
    for way in (*far_line, *far_cross):
        if way not in told:
            send_meta(*way)
    for way in batches[1]:
        send_tiles(*way)

    joins = []
    for u in range(1, near_heights):
        halves[u].wait_recv()
        for w, h in enumerate(heights(u)):
            for v in range(vblocks):
                at = u * span + w * vblocks + v
                asend[at] = summed(h, side, v) + precv[at]
        where = pl.ds(u * span, span)
        copy = remote(
            asend.at[where], arecv.at[where], xs, xr, (gx, beside(u) * 2 + side)
        )
        copy.start()
        joins.append(copy)
    for way in batches[2]:
        send_tiles(*way)

    halves[0].wait_recv()
    if joins:
        landed(arecv.at[pl.ds(span, len(joins) * span)], xr)

    def gathered(w, h, v):
        total = summed(h, side, v) + precv[w * vblocks + v]
        for u in range(1, near_heights):
            total = total + arecv[u * span + w * vblocks + v]
        return total

    mirror = nh - 1 - height
    for v in range(vblocks):
        term = gathered(1, mirror, v)
        peak = jnp.max(jnp.abs(term), axis=0, keepdims=True)
        small = peak < 2.0**-62
        term, peak = term * jnp.where(small, 2.0**64, 1.0), peak * jnp.where(small, 2.0**64, 1.0)
        term = term * jnp.where(peak > 0, 32767.0 / jnp.where(peak > 0, peak, 1.0), 0.0)
        term = (term + jnp.where(term < 0, -0.5, 0.5)).astype(jnp.int32)
        qsend[v] = term.astype(jnp.int16)
        ssend[v : v + 1, :] = peak * (1.0 / 32767.0)
        ssend[vblocks + v : vblocks + v + 1, :] = jnp.where(small, 2.0**-64, 1.0)
    owner = (gx, mirror * 2 + side)
    partials = [
        remote(ssend, srecv, qs.at[0], qr.at[0], owner),
        remote(qsend, qrecv, qs.at[1], qr.at[1], owner),
    ]
    for copy in partials:
        copy.start()
    for way in batches[3]:
        send_tiles(*way)

    own = [gathered(0, height, v) for v in range(vblocks)]
    for d in range(1, half):
        c = near(half - d)
        pl.when(~needed(c))(meta(c, c, d).wait_recv)
    landed(mbuf.at[pl.ds(0, half)], mr.at[0])
    count = [jnp.sum((mbuf[c, 0:1, :] > 0).astype(jnp.int32)) for c in range(ny)]
    first = [jnp.int32(0)]
    for c in range(ny - 1):
        first.append(first[-1] + count[c])
    table_ref[...] = jnp.zeros(table_ref.shape, jnp.int32)
    slot = lax.broadcasted_iota(jnp.int32, (1, 128), 1)
    wanted = slot * ny + gy
    at = jnp.full((1, 128), slots, jnp.int32)
    for c in range(ny):
        offset = c * share + (gy - first[c] + slots * ny) // ny - slots
        here = (wanted >= first[c]) & (wanted < first[c] + count[c])
        at = jnp.where(here, slot + offset, at)
    links[0:1, :] = at
    placing = pltpu.make_async_copy(links, slinks, isem)
    placing.start()
    lane = lax.broadcasted_iota(jnp.int32, (owned, 128), 1)
    line = lax.broadcasted_iota(jnp.int32, (owned, 128), 0)
    wanted = line * ny + gy
    sums = [jnp.zeros((owned, 128), jnp.int32) for _ in range(3)]
    for c in range(ny):
        work = mbuf[c, 0:1, :]
        hit = (lane + first[c] == wanted) & (work > 0)
        for i in range(3):
            sums[i] = sums[i] + jnp.where(hit, mbuf[c, i : i + 1, :], 0)
    for i in range(3):
        column = jnp.sum(sums[i], axis=1, keepdims=True)
        spread = jnp.where(line == lane, jnp.broadcast_to(column, (owned, 128)), 0)
        table_ref[i : i + 1, :] = jnp.sum(spread, axis=0, keepdims=True)

    placing.wait()
    for copy in partials:
        copy.wait_recv()
    for v in range(vblocks):
        coded = qrecv[v].astype(jnp.int32).astype(jnp.float32)
        scale = srecv[v : v + 1, :]
        prod_ref[v] = own[v] + coded * scale * srecv[vblocks + v : vblocks + v + 1, :]
    landed(recv.at[pl.ds(0, (ny - 1) * share)], tr)

    def settle(s, carry):
        moved_ref[s] = recv[slinks[0, s]]
        return carry

    lax.fori_loop(0, owned, settle, 0, unroll=4)
    landed(mbuf.at[pl.ds(0, ny - 1)], ms)
    landed(fbuf.at[pl.ds(0, (nx - 1) * vblocks)], fs)
    landed(stage.at[pl.ds(0, (ny - 1) * share)], ts)
    landed(psend, ps)
    if joins:
        landed(asend.at[pl.ds(span, len(joins) * span)], xs)
    for copy in partials:
        copy.wait_send()


def deliver(owned, meta_ref, prod_ref, moved_ref, prod_out, moved_out, row_out, col_out, work_out, lists, sems):
    outs = [(moved_ref, moved_out), (prod_ref, prod_out)]
    for i, ref in enumerate((work_out, row_out, col_out)):
        lists[i] = meta_ref[i, 0:owned]
        outs.append((lists.at[i], ref))
    copies = [pltpu.make_async_copy(*pair, sems.at[i]) for i, pair in enumerate(outs)]
    for copy in copies:
        copy.start()
    for copy in copies:
        copy.wait()


def size(shape, kind):
    total = jnp.dtype(kind).itemsize
    for extent in shape:
        total *= extent
    return total


def on_device(nx, ny, features, tile_vals, tile_row, tile_col, tile_work):
    slots, order = tile_vals.shape[:2]
    width = features.shape[1]
    vblocks = features.shape[0] // order
    owned = slots // 2
    near_heights = ny // 4
    half_blocks = near_heights * 2 * vblocks
    vmem = pl.BlockSpec(memory_space=pltpu.VMEM)
    anywhere = pl.BlockSpec(memory_space=pl.ANY)
    hbm = pl.BlockSpec(memory_space=pltpu.HBM)
    bf, f32, i32 = jnp.bfloat16, jnp.float32, jnp.int32
    dma = pltpu.SemaphoreType.DMA
    buffers = [
        ((slots, order, order), bf),
        ((slots, order, order), bf),
        ((slots + 1, order, order), bf),
        ((nx * vblocks, order, width), bf),
        ((ny, 4, 128), i32),
        ((1, 128), i32),
        ((8, 128), i32),
        None,
        ((slots + 1, order, width), f32),
        ((half_blocks, order, width), f32),
        ((half_blocks, order, width), f32),
        ((half_blocks, order, width), f32),
        ((half_blocks, order, width), f32),
        ((vblocks, order, width), jnp.int16),
        ((vblocks, order, width), jnp.int16),
        ((2 * vblocks, width), f32),
        ((2 * vblocks, width), f32),
    ]
    results = (
        jax.ShapeDtypeStruct((vblocks, order, width), f32),
        jax.ShapeDtypeStruct((owned, order, order), bf),
        jax.ShapeDtypeStruct((8, 128), i32),
    )
    need = sum(size(*b) for b in buffers if b) + sum(size(r.shape, r.dtype) for r in results)
    product, moved, table = pl.pallas_call(
        functools.partial(exchange, nx, ny, slots, vblocks, owned),
        out_shape=results,
        in_specs=[hbm] * 5,
        out_specs=(vmem, vmem, vmem),
        scratch_shapes=[
            pltpu.VMEM(*b) if b else pltpu.SMEM((8, 128), i32) for b in buffers
        ] + [
            pltpu.SMEM((slots,), i32),
            pltpu.SMEM((slots,), i32),
            pltpu.VMEM((slots,), i32),
            pltpu.VMEM((slots,), i32),
            pltpu.VMEM((slots,), i32),
            pltpu.VMEM((vblocks, order, width), bf),
            pltpu.SemaphoreType.REGULAR((ny,)), pltpu.SemaphoreType.REGULAR((nx,)),
            dma, dma, dma((6,)), dma, dma((ny // 2,)), dma, dma,
            dma, dma, dma, dma((near_heights,)), dma, dma, dma((2,)), dma((2,)),
        ],
        compiler_params=pltpu.CompilerParams(
            collective_id=0, has_side_effects=True, vmem_limit_bytes=need + 4 * 2**20
        ),
    )(*(
        pltpu.with_memory_space_constraint(x, pltpu.HBM)
        for x in (
            tile_work, tile_row, tile_col,
            features.reshape(vblocks, order, width), tile_vals,
        )
    ))
    index = jax.ShapeDtypeStruct((owned,), i32)
    product, moved, row, col, work = pl.pallas_call(
        functools.partial(deliver, owned),
        out_shape=(
            jax.ShapeDtypeStruct((vblocks, order, width), f32),
            jax.ShapeDtypeStruct((owned, order, order), bf),
            index, index, index,
        ),
        in_specs=[vmem, vmem, vmem],
        out_specs=(hbm,) * 5,
        scratch_shapes=[pltpu.VMEM((3, owned), i32), dma((5,))],
        compiler_params=pltpu.CompilerParams(vmem_limit_bytes=4 * 2**20),
    )(table, product, moved)
    return product.reshape(vblocks * order, width), moved, row, col, work


def solution(mesh):
    both = ("gx", "gy")
    return jax.shard_map(
        functools.partial(on_device, mesh.shape["gx"], mesh.shape["gy"]),
        mesh=mesh,
        in_specs=(P(both, None), P(both, None, None), P(both), P(both), P(both)),
        out_specs=(P(both, None), P(both, None, None), P(both), P(both), P(both)),
        check_vma=False,
    )
```

```python
import functools

import jax
import jax.numpy as jnp
from jax import lax
from jax.experimental import pallas as pl
from jax.experimental.pallas import tpu as pltpu
from jax.sharding import PartitionSpec as P

MESH = pl.DeviceIdType.MESH
LENT = 32


def exchange(
    nx, ny, slots, vblocks, owned,
    work_in, row_in, col_in, feat_in, vals_ref,
    prod_ref, moved_ref, table_ref,
    vbuf, stage, recv, fbuf, mbuf, live_ref, links, slinks, prefix,
    psend, precv, asend, arecv, qsend, qrecv, carried, ssend, srecv,
    swork_ref, scol_ref, work_ref, row_ref, col_ref, ready, xready,
    lsem, isem, insem, ms, mr, fs, fr, ts, tr, ps, pr, xs, xr, qs, qr, cs, cr,
):
    share = slots // ny
    half = ny // 2
    nh = ny // 2
    near_heights = nh // 2
    order = feat_in.shape[1]
    gx, gy = lax.axis_index("gx"), lax.axis_index("gy")
    side, height = lax.rem(gy, 2), gy // 2
    upper, place_in_half = gy // half, lax.rem(gy, half)
    base = upper * half

    load = pltpu.make_async_copy(vals_ref, vbuf, lsem)
    fetches = [
        pltpu.make_async_copy(src, dst, insem.at[i])
        for i, (src, dst) in enumerate((
            (work_in, work_ref), (row_in, row_ref), (col_in, col_ref),
            (feat_in, fbuf.at[pl.ds(0, vblocks)]),
            (work_in, swork_ref), (col_in, scol_ref),
        ))
    ]
    for copy in fetches:
        copy.start()
    load.start()

    def near(d):
        return base + lax.rem(place_in_half + d, half)

    def around(d):
        return lax.rem(gy + d, ny)

    def along_x(d):
        return lax.rem(gx + d, nx)

    def remote(src, dst, send, arrive, where):
        return pltpu.make_async_remote_copy(
            src_ref=src, dst_ref=dst, send_sem=send, recv_sem=arrive,
            device_id=where, device_id_type=MESH,
        )

    def landed(ref, sem):
        pltpu.make_async_copy(ref, ref, sem).wait()

    def signal(sem, where):
        pl.semaphore_signal(sem, inc=1, device_id=where, device_id_type=MESH)

    def rank(c):
        return (c // 2 + lax.rem(c, 2)) * ny + c

    mine = rank(gy)

    def above(e):
        return rank(e) > mine

    def below(e):
        return rank(e) < mine

    lower = gx
    for d in range(1, ny):
        lower = lower + jnp.where(below(around(d)), 1, 0)
    barrier = pltpu.get_barrier_semaphore()
    for d in range(1, ny):
        pl.when(above(around(d)))(functools.partial(signal, barrier, (gx, around(d))))
    for d in range(1, nx):
        pl.when(along_x(d) > gx)(functools.partial(signal, barrier, (along_x(d), gy)))
    mbuf[gy] = jnp.zeros(mbuf.shape[1:], jnp.int32)
    recv[slots] = jnp.zeros(recv.shape[1:], recv.dtype)
    pl.when(lower > 0)(lambda: pl.semaphore_wait(barrier, lower))
    for d in range(1, ny):
        pl.when(below(around(d)))(functools.partial(signal, ready.at[gy], (gx, around(d))))
    for d in range(1, nx):
        pl.when(along_x(d) < gx)(functools.partial(signal, xready.at[gx], (along_x(d), gy)))
    for copy in fetches:
        copy.wait()
    for i, ref in enumerate((work_ref, row_ref, col_ref)):
        mbuf[gy, i : i + 1, 0:slots] = ref[...].reshape(1, slots)

    def answered(e):
        pl.when(above(e))(lambda: pl.semaphore_wait(ready.at[e], 1))

    def meta(c, e, i):
        return remote(mbuf.at[c], mbuf.at[c], ms, mr.at[i], (gx, e))

    metas = [meta(gy, near(d), d) for d in range(1, half)]
    for d in range(half - 1, 0, -1):
        pl.when(below(near(d)))(metas[d - 1].start)
    feats = [
        remote(
            fbuf.at[pl.ds(0, vblocks)], fbuf.at[pl.ds(d * vblocks, vblocks)], fs, fr,
            (along_x(d), gy),
        )
        for d in range(1, nx)
    ]
    for d in range(1, nx):
        pl.when(along_x(d) < gx)(feats[d - 1].start)
    for d in range(1, half):
        answered(near(d))
        pl.when(above(near(d)))(metas[d - 1].start)

    at_end = (gy == 0) | (upper > 0)

    def share_features(now):
        for d in range(1, nx):
            @pl.when(now & (along_x(d) > gx))
            def _(d=d):
                pl.semaphore_wait(xready.at[along_x(d)], 1)
                feats[d - 1].start()

    share_features(~at_end)

    def needed(c):
        return jnp.where(upper > 0, c > gy, c < gy)

    def alive(c):
        return (mbuf[c, 0:1, :] > 0).astype(jnp.int32)

    live_ref[...] = alive(gy) * jnp.where(upper > 0, 1, 0)
    for d in range(1, half):
        @pl.when(needed(near(half - d)))
        def _(c=near(half - d), d=d):
            meta(c, c, d).wait_recv()
            live_ref[...] += alive(c)
    passed = jnp.sum(live_ref[...])
    start = lax.rem(jnp.where(upper > 0, ny * owned - passed, passed), ny)

    load.wait()
    def target(across, up, over):
        h = (1 - upper if across else upper) * near_heights + lax.rem(
            lax.rem(height, near_heights) + up, near_heights
        )
        return h * 2 + (1 - side if over else side)

    def send_tiles(across, up, over, low=0, high=share):
        e = target(across, up, over)
        if across and low == 0:
            answered(e)
        if (across, up, over, low) == (1, 0, 0, 0):
            meta(gy, e, 0).start()
        i = (across * near_heights + up) * 2 + over
        shift = lax.rem(e + ny - start, ny)
        for k in range(low, high):
            stage[i * share + k] = vbuf[k * ny + shift]
        remote(
            stage.at[pl.ds(i * share + low, high - low)],
            recv.at[pl.ds(gy * share + low, high - low)],
            ts, tr, (gx, e),
        ).start()

    def cut(ways, low, high):
        return [(*way, low, high) for way in ways]

    mate = target(1, 0, 0)
    near_line = [(0, u, 0) for u in range(1, near_heights)]
    near_cross = [(0, u, 1) for u in range(1, near_heights)]
    far_line = [(1, u, 0) for u in range(near_heights)]
    far_cross = [(1, u, 1) for u in range(near_heights)]
    pair = [(0, 0, 1)]
    middle = near_heights // 2
    batches = [far_line[:middle] + near_line + pair + far_line[middle:], far_cross[:middle], far_cross[middle:] + near_cross, []]
    for way in batches[0]:
        send_tiles(*way)
    share_features(at_end)
    shift = lax.rem(gy + ny - start, ny)
    for k in range(share):
        recv[gy * share + k] = vbuf[k * ny + shift]

    prefix[slots] = jnp.zeros(prefix.shape[1:], jnp.float32)
    down = lax.broadcasted_iota(jnp.int32, (128, 128), 0)
    across = lax.broadcasted_iota(jnp.int32, (128, 128), 1)
    rows = jnp.where(across < slots, mbuf[gy, 1:2, :] - gx * (ny * vblocks), -1)
    upright = jnp.sum(jnp.where(down == across, rows, 0), axis=1, keepdims=True)
    prev = jnp.max(
        jnp.where((upright == rows) & (down < across), down, -1), axis=0, keepdims=True
    )
    last = jnp.max(jnp.where(upright == across, down, -1), axis=0, keepdims=True)
    links[...] = jnp.zeros((8, 128), jnp.int32)
    links[0:1, :] = jnp.where(prev < 0, slots, prev)
    links[1:2, :] = jnp.where(last < 0, slots, last)
    listing = pltpu.make_async_copy(links, slinks, isem)
    listing.start()
    listing.wait()
    landed(fbuf.at[pl.ds(vblocks, (nx - 1) * vblocks)], fr)
    pattern = lax.broadcasted_iota(jnp.int32, (order, order), 0) * order + lax.broadcasted_iota(
        jnp.int32, (order, order), 1
    )
    group = 4

    def multiply(step, carry):
        terms = []
        for u in range(group):
            t = step * group + u
            values = vbuf[t].astype(jnp.float32)
            masked = jnp.where(pattern < swork_ref[t], values, 0.0).astype(jnp.bfloat16)
            col = scol_ref[t]
            back = lax.rem(gx - col // vblocks // ny + nx, nx)
            block = fbuf[back * vblocks + lax.rem(col, vblocks)]
            terms.append(jnp.dot(masked, block, preferred_element_type=jnp.float32))
        for u in range(group):
            t = step * group + u
            prefix[t] = terms[u] + prefix[slinks[0, t]]
        return carry

    lax.fori_loop(0, slots // group, multiply, 0)

    meta(mate, mate, 0).wait_recv()
    for d in range(1, half):
        remote(mbuf.at[mate], mbuf.at[mate], ms, mr.at[half], (gx, near(d))).start()

    def summed(h, q, v):
        return prefix[slinks[1, (h * 2 + q) * vblocks + v]]

    def beside(u):
        return upper * near_heights + lax.rem(lax.rem(height, near_heights) + u, near_heights)

    def heights(u):
        h = beside(u)
        return (h, nh - 1 - h)

    span = 2 * vblocks
    halves = {}
    for u in [*range(1, near_heights), 0]:
        for w, h in enumerate(heights(u)):
            for v in range(vblocks):
                psend[u * span + w * vblocks + v] = summed(h, 1 - side, v)
        where = pl.ds(u * span, span)
        copy = remote(
            psend.at[where], precv.at[where], ps, pr.at[u], (gx, gy + 1 - 2 * side)
        )
        copy.start()
        halves[u] = copy
    for way in batches[1]:
        send_tiles(*way)

    joins = []
    for u in range(1, near_heights):
        halves[u].wait_recv()
        for w, h in enumerate(heights(u)):
            for v in range(vblocks):
                at = u * span + w * vblocks + v
                asend[at] = summed(h, side, v) + precv[at]
        where = pl.ds(u * span, span)
        copy = remote(
            asend.at[where], arecv.at[where], xs, xr, (gx, beside(u) * 2 + side)
        )
        copy.start()
        joins.append(copy)
    for way in batches[2]:
        send_tiles(*way)

    halves[0].wait_recv()
    if joins:
        landed(arecv.at[pl.ds(span, len(joins) * span)], xr)

    def gathered(w, h, v):
        total = summed(h, side, v) + precv[w * vblocks + v]
        for u in range(1, near_heights):
            total = total + arecv[u * span + w * vblocks + v]
        return total

    mirror = nh - 1 - height
    for v in range(vblocks):
        term = gathered(1, mirror, v)
        peak = jnp.max(jnp.abs(term), axis=0, keepdims=True)
        small = peak < 2.0**-62
        term, peak = term * jnp.where(small, 2.0**64, 1.0), peak * jnp.where(small, 2.0**64, 1.0)
        term = term * jnp.where(peak > 0, 32767.0 / jnp.where(peak > 0, peak, 1.0), 0.0)
        term = (term + jnp.where(term < 0, -0.5, 0.5)).astype(jnp.int32)
        qsend[pl.ds(v * order, order)] = term.astype(jnp.int16)
        ssend[v : v + 1, :] = peak * (1.0 / 32767.0)
        ssend[vblocks + v : vblocks + v + 1, :] = jnp.where(small, 2.0**-64, 1.0)
    owner = (gx, mirror * 2 + side)
    tail = order * LENT // 128
    body, end = pl.ds(0, vblocks * order - tail), pl.ds(vblocks * order - tail, tail)
    lends, carries = (upper > 0) & (side == 0), (upper > 0) & (side == 1)
    partials = [
        remote(ssend, srecv, qs.at[0], qr.at[0], owner),
        remote(qsend.at[body], qrecv.at[body], qs.at[1], qr.at[1], owner),
    ]
    for copy in partials:
        copy.start()
    direct = remote(qsend.at[end], qrecv.at[end], qs.at[2], qr.at[2], owner)
    lent = remote(qsend.at[end], carried, qs.at[2], cr, (gx, lax.rem(gy + 1, ny)))
    carry_on = remote(carried, qrecv.at[end], cs, qr.at[2], (gx, lax.rem(mirror * 2 + 1 - side, ny)))
    pl.when(~lends)(direct.start)
    pl.when(lends)(lent.start)
    for way in batches[3]:
        send_tiles(*way)

    @pl.when(carries)
    def _():
        lent.wait_recv()
        carry_on.start()


    own = [gathered(0, height, v) for v in range(vblocks)]
    for d in range(1, half):
        c = near(half - d)
        pl.when(~needed(c))(meta(c, c, d).wait_recv)
    landed(mbuf.at[pl.ds(0, half - 1)], mr.at[half])
    count = [jnp.sum((mbuf[c, 0:1, :] > 0).astype(jnp.int32)) for c in range(ny)]
    first = [jnp.int32(0)]
    for c in range(ny - 1):
        first.append(first[-1] + count[c])
    table_ref[...] = jnp.zeros(table_ref.shape, jnp.int32)
    slot = lax.broadcasted_iota(jnp.int32, (1, 128), 1)
    wanted = slot * ny + gy
    at = jnp.full((1, 128), slots, jnp.int32)
    for c in range(ny):
        offset = c * share + (gy - first[c] + slots * ny) // ny - slots
        here = (wanted >= first[c]) & (wanted < first[c] + count[c])
        at = jnp.where(here, slot + offset, at)
    links[0:1, :] = at
    placing = pltpu.make_async_copy(links, slinks, isem)
    placing.start()
    lane = lax.broadcasted_iota(jnp.int32, (owned, 128), 1)
    line = lax.broadcasted_iota(jnp.int32, (owned, 128), 0)
    wanted = line * ny + gy
    sums = [jnp.zeros((owned, 128), jnp.int32) for _ in range(3)]
    for c in range(ny):
        work = mbuf[c, 0:1, :]
        hit = (lane + first[c] == wanted) & (work > 0)
        for i in range(3):
            sums[i] = sums[i] + jnp.where(hit, mbuf[c, i : i + 1, :], 0)
    for i in range(3):
        column = jnp.sum(sums[i], axis=1, keepdims=True)
        spread = jnp.where(line == lane, jnp.broadcast_to(column, (owned, 128)), 0)
        table_ref[i : i + 1, :] = jnp.sum(spread, axis=0, keepdims=True)

    placing.wait()
    for copy in (*partials, direct):
        copy.wait_recv()
    for v in range(vblocks):
        coded = qrecv[pl.ds(v * order, order)].astype(jnp.int32).astype(jnp.float32)
        scale = srecv[v : v + 1, :]
        prod_ref[v] = own[v] + coded * scale * srecv[vblocks + v : vblocks + v + 1, :]
    landed(recv.at[pl.ds(0, (ny - 1) * share)], tr)

    def settle(s, carry):
        moved_ref[s] = recv[slinks[0, s]]
        return carry

    lax.fori_loop(0, owned, settle, 0, unroll=4)
    landed(mbuf.at[pl.ds(0, ny - 1)], ms)
    landed(fbuf.at[pl.ds(0, (nx - 1) * vblocks)], fs)
    landed(stage.at[pl.ds(0, (ny - 1) * share)], ts)
    landed(psend, ps)
    if joins:
        landed(asend.at[pl.ds(span, len(joins) * span)], xs)
    for copy in (*partials, direct):
        copy.wait_send()
    pl.when(carries)(carry_on.wait_send)


def deliver(owned, meta_ref, prod_ref, moved_ref, prod_out, moved_out, row_out, col_out, work_out, lists, sems):
    part = owned // 1
    outs = [(prod_ref, prod_out)]
    for i in range(1):
        where = pl.ds(i * part, part)
        outs.append((moved_ref.at[where], moved_out.at[where]))
    for i, ref in enumerate((work_out, row_out, col_out)):
        lists[i] = meta_ref[i, 0:owned]
        outs.append((lists.at[i], ref))
    copies = [pltpu.make_async_copy(*pair, sems.at[i]) for i, pair in enumerate(outs)]
    for copy in copies:
        copy.start()
    for copy in copies:
        copy.wait()


def size(shape, kind):
    total = jnp.dtype(kind).itemsize
    for extent in shape:
        total *= extent
    return total


def on_device(nx, ny, features, tile_vals, tile_row, tile_col, tile_work):
    slots, order = tile_vals.shape[:2]
    width = features.shape[1]
    vblocks = features.shape[0] // order
    owned = slots // 2
    near_heights = ny // 4
    half_blocks = near_heights * 2 * vblocks
    vmem = pl.BlockSpec(memory_space=pltpu.VMEM)
    anywhere = pl.BlockSpec(memory_space=pl.ANY)
    hbm = pl.BlockSpec(memory_space=pltpu.HBM)
    bf, f32, i32 = jnp.bfloat16, jnp.float32, jnp.int32
    dma = pltpu.SemaphoreType.DMA
    buffers = [
        ((slots, order, order), bf),
        ((slots, order, order), bf),
        ((slots + 1, order, order), bf),
        ((nx * vblocks, order, width), bf),
        ((ny, 4, 128), i32),
        ((1, 128), i32),
        ((8, 128), i32),
        None,
        ((slots + 1, order, width), f32),
        ((half_blocks, order, width), f32),
        ((half_blocks, order, width), f32),
        ((half_blocks, order, width), f32),
        ((half_blocks, order, width), f32),
        ((vblocks * order, width), jnp.int16),
        ((vblocks * order, width), jnp.int16),
        ((order * LENT // 128, width), jnp.int16),
        ((2 * vblocks, width), f32),
        ((2 * vblocks, width), f32),
    ]
    results = (
        jax.ShapeDtypeStruct((vblocks, order, width), f32),
        jax.ShapeDtypeStruct((owned, order, order), bf),
        jax.ShapeDtypeStruct((8, 128), i32),
    )
    need = sum(size(*b) for b in buffers if b) + sum(size(r.shape, r.dtype) for r in results)
    product, moved, table = pl.pallas_call(
        functools.partial(exchange, nx, ny, slots, vblocks, owned),
        out_shape=results,
        in_specs=[hbm] * 5,
        out_specs=(vmem, vmem, vmem),
        scratch_shapes=[
            pltpu.VMEM(*b) if b else pltpu.SMEM((8, 128), i32) for b in buffers
        ] + [
            pltpu.SMEM((slots,), i32),
            pltpu.SMEM((slots,), i32),
            pltpu.VMEM((slots,), i32),
            pltpu.VMEM((slots,), i32),
            pltpu.VMEM((slots,), i32),
            pltpu.SemaphoreType.REGULAR((ny,)), pltpu.SemaphoreType.REGULAR((nx,)),
            dma, dma, dma((6,)), dma, dma((ny // 2 + 1,)), dma, dma,
            dma, dma, dma, dma((near_heights,)), dma, dma, dma((3,)), dma((3,)), dma, dma,
        ],
        compiler_params=pltpu.CompilerParams(
            collective_id=0, has_side_effects=True, vmem_limit_bytes=need + 4 * 2**20
        ),
    )(*(
        pltpu.with_memory_space_constraint(x, pltpu.HBM)
        for x in (
            tile_work, tile_row, tile_col,
            features.reshape(vblocks, order, width), tile_vals,
        )
    ))
    index = jax.ShapeDtypeStruct((owned,), i32)
    product, moved, row, col, work = pl.pallas_call(
        functools.partial(deliver, owned),
        out_shape=(
            jax.ShapeDtypeStruct((vblocks, order, width), f32),
            jax.ShapeDtypeStruct((owned, order, order), bf),
            index, index, index,
        ),
        in_specs=[vmem, vmem, vmem],
        out_specs=(hbm,) * 5,
        scratch_shapes=[pltpu.VMEM((3, owned), i32), dma((4 + 1,))],
        compiler_params=pltpu.CompilerParams(vmem_limit_bytes=4 * 2**20),
    )(table, product, moved)
    return product.reshape(vblocks * order, width), moved, row, col, work


def solution(mesh):
    both = ("gx", "gy")
    return jax.shard_map(
        functools.partial(on_device, mesh.shape["gx"], mesh.shape["gy"]),
        mesh=mesh,
        in_specs=(P(both, None), P(both, None, None), P(both), P(both), P(both)),
        out_specs=(P(both, None), P(both, None, None), P(both), P(both), P(both)),
        check_vma=False,
    )
```

```python
import functools

import jax
import jax.numpy as jnp
from jax import lax
from jax.experimental import pallas as pl
from jax.experimental.pallas import tpu as pltpu
from jax.sharding import PartitionSpec as P

MESH = pl.DeviceIdType.MESH
LENT = 64


def exchange(
    nx, ny, slots, vblocks, owned,
    work_in, row_in, col_in, feat_in, vals_ref,
    prod_ref, moved_ref, table_ref,
    vbuf0, vbuf1, stage, recv, fbuf, mbuf, live_ref, links, slinks, prefix,
    psend, precv, asend, arecv, qsend, qrecv, carried, ssend, srecv,
    swork_ref, scol_ref, work_ref, row_ref, col_ref, ready, xready,
    lsem, isem, insem, ms, mr, fs, fr, ts, tr, ps, pr, xs, xr, qs, qr, cs, cr,
):
    share = slots // ny
    half = ny // 2
    nh = ny // 2
    near_heights = nh // 2
    order = feat_in.shape[1]
    gx, gy = lax.axis_index("gx"), lax.axis_index("gy")
    side, height = lax.rem(gy, 2), gy // 2
    upper, place_in_half = gy // half, lax.rem(gy, half)
    base = upper * half

    held = (vbuf0, vbuf1)
    piece = slots // len(held)
    loads = [
        pltpu.make_async_copy(vals_ref.at[pl.ds(i * piece, piece)], ref, lsem.at[i])
        for i, ref in enumerate(held)
    ]
    fetches = [
        pltpu.make_async_copy(src, dst, insem.at[i])
        for i, (src, dst) in enumerate((
            (work_in, work_ref), (row_in, row_ref), (col_in, col_ref),
            (feat_in, fbuf.at[pl.ds(0, vblocks)]),
            (work_in, swork_ref), (col_in, scol_ref),
        ))
    ]
    for copy in fetches:
        copy.start()
    for copy in loads:
        copy.start()

    def near(d):
        return base + lax.rem(place_in_half + d, half)

    def around(d):
        return lax.rem(gy + d, ny)

    def along_x(d):
        return lax.rem(gx + d, nx)

    def remote(src, dst, send, arrive, where):
        return pltpu.make_async_remote_copy(
            src_ref=src, dst_ref=dst, send_sem=send, recv_sem=arrive,
            device_id=where, device_id_type=MESH,
        )

    def landed(ref, sem):
        pltpu.make_async_copy(ref, ref, sem).wait()

    def signal(sem, where):
        pl.semaphore_signal(sem, inc=1, device_id=where, device_id_type=MESH)

    def rank(c):
        return (c // 2 + lax.rem(c, 2)) * ny + c

    mine = rank(gy)

    def above(e):
        return rank(e) > mine

    def below(e):
        return rank(e) < mine

    lower = gx
    for d in range(1, ny):
        lower = lower + jnp.where(below(around(d)), 1, 0)
    barrier = pltpu.get_barrier_semaphore()
    for d in range(1, ny):
        pl.when(above(around(d)))(functools.partial(signal, barrier, (gx, around(d))))
    for d in range(1, nx):
        pl.when(along_x(d) > gx)(functools.partial(signal, barrier, (along_x(d), gy)))
    mbuf[gy] = jnp.zeros(mbuf.shape[1:], jnp.int32)
    recv[slots] = jnp.zeros(recv.shape[1:], recv.dtype)
    pl.when(lower > 0)(lambda: pl.semaphore_wait(barrier, lower))
    for d in range(1, ny):
        pl.when(below(around(d)))(functools.partial(signal, ready.at[gy], (gx, around(d))))
    for d in range(1, nx):
        pl.when(along_x(d) < gx)(functools.partial(signal, xready.at[gx], (along_x(d), gy)))
    for copy in fetches:
        copy.wait()
    for i, ref in enumerate((work_ref, row_ref, col_ref)):
        mbuf[gy, i : i + 1, 0:slots] = ref[...].reshape(1, slots)

    def answered(e):
        pl.when(above(e))(lambda: pl.semaphore_wait(ready.at[e], 1))

    def meta(c, e, i):
        return remote(mbuf.at[c], mbuf.at[c], ms, mr.at[i], (gx, e))

    metas = [meta(gy, near(d), d) for d in range(1, half)]
    for d in range(half - 1, 0, -1):
        pl.when(below(near(d)))(metas[d - 1].start)
    feats = [
        remote(
            fbuf.at[pl.ds(0, vblocks)], fbuf.at[pl.ds(d * vblocks, vblocks)], fs, fr,
            (along_x(d), gy),
        )
        for d in range(1, nx)
    ]
    for d in range(1, nx):
        pl.when(along_x(d) < gx)(feats[d - 1].start)
    for d in range(1, half):
        answered(near(d))
        pl.when(above(near(d)))(metas[d - 1].start)

    at_end = (gy == 0) | (upper > 0)

    def share_features(now):
        for d in range(1, nx):
            @pl.when(now & (along_x(d) > gx))
            def _(d=d):
                pl.semaphore_wait(xready.at[along_x(d)], 1)
                feats[d - 1].start()

    share_features(~at_end)

    def needed(c):
        return jnp.where(upper > 0, c > gy, c < gy)

    def alive(c):
        return (mbuf[c, 0:1, :] > 0).astype(jnp.int32)

    live_ref[...] = alive(gy) * jnp.where(upper > 0, 1, 0)
    for d in range(1, half):
        @pl.when(needed(near(half - d)))
        def _(c=near(half - d), d=d):
            meta(c, c, d).wait_recv()
            live_ref[...] += alive(c)
    passed = jnp.sum(live_ref[...])
    start = lax.rem(jnp.where(upper > 0, ny * owned - passed, passed), ny)

    loads[0].wait()
    def target(across, up, over):
        h = (1 - upper if across else upper) * near_heights + lax.rem(
            lax.rem(height, near_heights) + up, near_heights
        )
        return h * 2 + (1 - side if over else side)

    def tile_at(k, shift):
        return held[k * ny // piece][k * ny % piece + shift]

    def send_tiles(across, up, over, low=0, high=share):
        e = target(across, up, over)
        if across and low == 0:
            answered(e)
        if (across, up, over, low) == (1, 0, 0, 0):
            meta(gy, e, 0).start()
        i = (across * near_heights + up) * 2 + over
        shift = lax.rem(e + ny - start, ny)
        for k in range(low, high):
            stage[i * share + k] = tile_at(k, shift)
        remote(
            stage.at[pl.ds(i * share + low, high - low)],
            recv.at[pl.ds(gy * share + low, high - low)],
            ts, tr, (gx, e),
        ).start()

    def cut(ways, low, high):
        return [(*way, low, high) for way in ways]

    mate = target(1, 0, 0)
    near_line = [(0, u, 0) for u in range(1, near_heights)]
    near_cross = [(0, u, 1) for u in range(1, near_heights)]
    far_line = [(1, u, 0) for u in range(near_heights)]
    far_cross = [(1, u, 1) for u in range(near_heights)]
    pair = [(0, 0, 1)]
    middle = near_heights // 2
    batches = [far_line[:middle] + near_line + pair + far_line[middle:], far_cross[:middle], near_cross + far_cross[middle:], []]
    send_tiles(*batches[0][0], 0, share // 2)
    loads[1].wait()
    send_tiles(*batches[0][0], share // 2, share)
    for way in batches[0][1:]:
        send_tiles(*way)
    share_features(at_end)
    shift = lax.rem(gy + ny - start, ny)
    for k in range(share):
        recv[gy * share + k] = tile_at(k, shift)

    prefix[slots] = jnp.zeros(prefix.shape[1:], jnp.float32)
    down = lax.broadcasted_iota(jnp.int32, (128, 128), 0)
    across = lax.broadcasted_iota(jnp.int32, (128, 128), 1)
    rows = jnp.where(across < slots, mbuf[gy, 1:2, :] - gx * (ny * vblocks), -1)
    upright = jnp.sum(jnp.where(down == across, rows, 0), axis=1, keepdims=True)
    prev = jnp.max(
        jnp.where((upright == rows) & (down < across), down, -1), axis=0, keepdims=True
    )
    last = jnp.max(jnp.where(upright == across, down, -1), axis=0, keepdims=True)
    links[...] = jnp.zeros((8, 128), jnp.int32)
    links[0:1, :] = jnp.where(prev < 0, slots, prev)
    links[1:2, :] = jnp.where(last < 0, slots, last)
    listing = pltpu.make_async_copy(links, slinks, isem)
    listing.start()
    listing.wait()
    landed(fbuf.at[pl.ds(vblocks, (nx - 1) * vblocks)], fr)
    pattern = lax.broadcasted_iota(jnp.int32, (order, order), 0) * order + lax.broadcasted_iota(
        jnp.int32, (order, order), 1
    )
    group = 4

    def multiply(i, step, carry):
        terms = []
        for u in range(group):
            t = i * piece + step * group + u
            values = held[i][step * group + u].astype(jnp.float32)
            masked = jnp.where(pattern < swork_ref[t], values, 0.0).astype(jnp.bfloat16)
            col = scol_ref[t]
            back = lax.rem(gx - col // vblocks // ny + nx, nx)
            block = fbuf[back * vblocks + lax.rem(col, vblocks)]
            terms.append(jnp.dot(masked, block, preferred_element_type=jnp.float32))
        for u in range(group):
            t = i * piece + step * group + u
            prefix[t] = terms[u] + prefix[slinks[0, t]]
        return carry

    for i in range(len(held)):
        lax.fori_loop(0, piece // group, functools.partial(multiply, i), 0)

    meta(mate, mate, 0).wait_recv()
    for d in range(1, half):
        remote(mbuf.at[mate], mbuf.at[mate], ms, mr.at[half], (gx, near(d))).start()

    def summed(h, q, v):
        return prefix[slinks[1, (h * 2 + q) * vblocks + v]]

    def beside(u):
        return upper * near_heights + lax.rem(lax.rem(height, near_heights) + u, near_heights)

    def heights(u):
        h = beside(u)
        return (h, nh - 1 - h)

    span = 2 * vblocks
    halves = {}
    for u in [*range(1, near_heights), 0]:
        for w, h in enumerate(heights(u)):
            for v in range(vblocks):
                psend[u * span + w * vblocks + v] = summed(h, 1 - side, v)
        where = pl.ds(u * span, span)
        copy = remote(
            psend.at[where], precv.at[where], ps, pr.at[u], (gx, gy + 1 - 2 * side)
        )
        copy.start()
        halves[u] = copy
    for way in batches[1]:
        send_tiles(*way)

    joins = []
    for u in range(1, near_heights):
        halves[u].wait_recv()
        for w, h in enumerate(heights(u)):
            for v in range(vblocks):
                at = u * span + w * vblocks + v
                asend[at] = summed(h, side, v) + precv[at]
        where = pl.ds(u * span, span)
        copy = remote(
            asend.at[where], arecv.at[where], xs, xr, (gx, beside(u) * 2 + side)
        )
        copy.start()
        joins.append(copy)
    for way in batches[2]:
        send_tiles(*way)

    halves[0].wait_recv()
    if joins:
        landed(arecv.at[pl.ds(span, len(joins) * span)], xr)

    def gathered(w, h, v):
        total = summed(h, side, v) + precv[w * vblocks + v]
        for u in range(1, near_heights):
            total = total + arecv[u * span + w * vblocks + v]
        return total

    mirror = nh - 1 - height
    for v in range(vblocks):
        term = gathered(1, mirror, v)
        peak = jnp.max(jnp.abs(term), axis=0, keepdims=True)
        small = peak < 2.0**-62
        term, peak = term * jnp.where(small, 2.0**64, 1.0), peak * jnp.where(small, 2.0**64, 1.0)
        term = term * jnp.where(peak > 0, 32767.0 / jnp.where(peak > 0, peak, 1.0), 0.0)
        term = (term + jnp.where(term < 0, -0.5, 0.5)).astype(jnp.int32)
        qsend[pl.ds(v * order, order)] = term.astype(jnp.int16)
        ssend[v : v + 1, :] = peak * (1.0 / 32767.0)
        ssend[vblocks + v : vblocks + v + 1, :] = jnp.where(small, 2.0**-64, 1.0)
    owner = (gx, mirror * 2 + side)
    tail = order * LENT // 128
    body, end = pl.ds(0, vblocks * order - tail), pl.ds(vblocks * order - tail, tail)
    lends, carries = (upper > 0) & (side == 0), (upper > 0) & (side == 1)
    partials = [
        remote(ssend, srecv, qs.at[0], qr.at[0], owner),
        remote(qsend.at[body], qrecv.at[body], qs.at[1], qr.at[1], owner),
    ]
    direct = remote(qsend.at[end], qrecv.at[end], qs.at[2], qr.at[2], owner)
    lent = remote(qsend.at[end], carried, qs.at[2], cr, (gx, lax.rem(gy + 1, ny)))
    carry_on = remote(carried, qrecv.at[end], cs, qr.at[2], (gx, lax.rem(mirror * 2 + 1 - side, ny)))
    pl.when(lends)(lent.start)

    @pl.when(carries)
    def _():
        lent.wait_recv()
        carry_on.start()

    for copy in partials:
        copy.start()
    pl.when(~lends)(direct.start)
    for way in batches[3]:
        send_tiles(*way)


    own = [gathered(0, height, v) for v in range(vblocks)]
    for d in range(1, half):
        c = near(half - d)
        pl.when(~needed(c))(meta(c, c, d).wait_recv)
    landed(mbuf.at[pl.ds(0, half - 1)], mr.at[half])
    count = [jnp.sum((mbuf[c, 0:1, :] > 0).astype(jnp.int32)) for c in range(ny)]
    first = [jnp.int32(0)]
    for c in range(ny - 1):
        first.append(first[-1] + count[c])
    table_ref[...] = jnp.zeros(table_ref.shape, jnp.int32)
    slot = lax.broadcasted_iota(jnp.int32, (1, 128), 1)
    wanted = slot * ny + gy
    at = jnp.full((1, 128), slots, jnp.int32)
    for c in range(ny):
        offset = c * share + (gy - first[c] + slots * ny) // ny - slots
        here = (wanted >= first[c]) & (wanted < first[c] + count[c])
        at = jnp.where(here, slot + offset, at)
    links[0:1, :] = at
    placing = pltpu.make_async_copy(links, slinks, isem)
    placing.start()
    lane = lax.broadcasted_iota(jnp.int32, (owned, 128), 1)
    line = lax.broadcasted_iota(jnp.int32, (owned, 128), 0)
    wanted = line * ny + gy
    sums = [jnp.zeros((owned, 128), jnp.int32) for _ in range(3)]
    for c in range(ny):
        work = mbuf[c, 0:1, :]
        hit = (lane + first[c] == wanted) & (work > 0)
        for i in range(3):
            sums[i] = sums[i] + jnp.where(hit, mbuf[c, i : i + 1, :], 0)
    for i in range(3):
        column = jnp.sum(sums[i], axis=1, keepdims=True)
        spread = jnp.where(line == lane, jnp.broadcast_to(column, (owned, 128)), 0)
        table_ref[i : i + 1, :] = jnp.sum(spread, axis=0, keepdims=True)

    placing.wait()
    for copy in (*partials, direct):
        copy.wait_recv()
    for v in range(vblocks):
        coded = qrecv[pl.ds(v * order, order)].astype(jnp.int32).astype(jnp.float32)
        scale = srecv[v : v + 1, :]
        prod_ref[v] = own[v] + coded * scale * srecv[vblocks + v : vblocks + v + 1, :]
    landed(recv.at[pl.ds(0, (ny - 1) * share)], tr)

    def settle(s, carry):
        moved_ref[s] = recv[slinks[0, s]]
        return carry

    lax.fori_loop(0, owned, settle, 0, unroll=4)
    landed(mbuf.at[pl.ds(0, ny - 1)], ms)
    landed(fbuf.at[pl.ds(0, (nx - 1) * vblocks)], fs)
    landed(stage.at[pl.ds(0, (ny - 1) * share)], ts)
    landed(psend, ps)
    if joins:
        landed(asend.at[pl.ds(span, len(joins) * span)], xs)
    for copy in (*partials, direct):
        copy.wait_send()
    pl.when(carries)(carry_on.wait_send)


def deliver(owned, meta_ref, prod_ref, moved_ref, prod_out, moved_out, row_out, col_out, work_out, lists, sems):
    part = owned // 1
    outs = [(prod_ref, prod_out)]
    for i in range(1):
        where = pl.ds(i * part, part)
        outs.append((moved_ref.at[where], moved_out.at[where]))
    for i, ref in enumerate((work_out, row_out, col_out)):
        lists[i] = meta_ref[i, 0:owned]
        outs.append((lists.at[i], ref))
    copies = [pltpu.make_async_copy(*pair, sems.at[i]) for i, pair in enumerate(outs)]
    for copy in copies:
        copy.start()
    for copy in copies:
        copy.wait()


def size(shape, kind):
    total = jnp.dtype(kind).itemsize
    for extent in shape:
        total *= extent
    return total


def on_device(nx, ny, features, tile_vals, tile_row, tile_col, tile_work):
    slots, order = tile_vals.shape[:2]
    width = features.shape[1]
    vblocks = features.shape[0] // order
    owned = slots // 2
    near_heights = ny // 4
    half_blocks = near_heights * 2 * vblocks
    vmem = pl.BlockSpec(memory_space=pltpu.VMEM)
    anywhere = pl.BlockSpec(memory_space=pl.ANY)
    hbm = pl.BlockSpec(memory_space=pltpu.HBM)
    bf, f32, i32 = jnp.bfloat16, jnp.float32, jnp.int32
    dma = pltpu.SemaphoreType.DMA
    buffers = [
        ((slots // 2, order, order), bf),
        ((slots // 2, order, order), bf),
        ((slots, order, order), bf),
        ((slots + 1, order, order), bf),
        ((nx * vblocks, order, width), bf),
        ((ny, 4, 128), i32),
        ((1, 128), i32),
        ((8, 128), i32),
        None,
        ((slots + 1, order, width), f32),
        ((half_blocks, order, width), f32),
        ((half_blocks, order, width), f32),
        ((half_blocks, order, width), f32),
        ((half_blocks, order, width), f32),
        ((vblocks * order, width), jnp.int16),
        ((vblocks * order, width), jnp.int16),
        ((order * LENT // 128, width), jnp.int16),
        ((2 * vblocks, width), f32),
        ((2 * vblocks, width), f32),
    ]
    results = (
        jax.ShapeDtypeStruct((vblocks, order, width), f32),
        jax.ShapeDtypeStruct((owned, order, order), bf),
        jax.ShapeDtypeStruct((8, 128), i32),
    )
    need = sum(size(*b) for b in buffers if b) + sum(size(r.shape, r.dtype) for r in results)
    product, moved, table = pl.pallas_call(
        functools.partial(exchange, nx, ny, slots, vblocks, owned),
        out_shape=results,
        in_specs=[hbm] * 5,
        out_specs=(vmem, vmem, vmem),
        scratch_shapes=[
            pltpu.VMEM(*b) if b else pltpu.SMEM((8, 128), i32) for b in buffers
        ] + [
            pltpu.SMEM((slots,), i32),
            pltpu.SMEM((slots,), i32),
            pltpu.VMEM((slots,), i32),
            pltpu.VMEM((slots,), i32),
            pltpu.VMEM((slots,), i32),
            pltpu.SemaphoreType.REGULAR((ny,)), pltpu.SemaphoreType.REGULAR((nx,)),
            dma((2,)), dma, dma((6,)), dma, dma((ny // 2 + 1,)), dma, dma,
            dma, dma, dma, dma((near_heights,)), dma, dma, dma((3,)), dma((3,)), dma, dma,
        ],
        compiler_params=pltpu.CompilerParams(
            collective_id=0, has_side_effects=True, vmem_limit_bytes=need + 4 * 2**20
        ),
    )(*(
        pltpu.with_memory_space_constraint(x, pltpu.HBM)
        for x in (
            tile_work, tile_row, tile_col,
            features.reshape(vblocks, order, width), tile_vals,
        )
    ))
    index = jax.ShapeDtypeStruct((owned,), i32)
    product, moved, row, col, work = pl.pallas_call(
        functools.partial(deliver, owned),
        out_shape=(
            jax.ShapeDtypeStruct((vblocks, order, width), f32),
            jax.ShapeDtypeStruct((owned, order, order), bf),
            index, index, index,
        ),
        in_specs=[vmem, vmem, vmem],
        out_specs=(hbm,) * 5,
        scratch_shapes=[pltpu.VMEM((3, owned), i32), dma((4 + 1,))],
        compiler_params=pltpu.CompilerParams(vmem_limit_bytes=4 * 2**20),
    )(table, product, moved)
    return product.reshape(vblocks * order, width), moved, row, col, work


def solution(mesh):
    both = ("gx", "gy")
    return jax.shard_map(
        functools.partial(on_device, mesh.shape["gx"], mesh.shape["gy"]),
        mesh=mesh,
        in_specs=(P(both, None), P(both, None, None), P(both), P(both), P(both)),
        out_specs=(P(both, None), P(both, None, None), P(both), P(both), P(both)),
        check_vma=False,
    )
```

```python
import functools

import jax
import jax.numpy as jnp
from jax import lax
from jax.experimental import pallas as pl
from jax.experimental.pallas import tpu as pltpu
from jax.sharding import PartitionSpec as P

MESH = pl.DeviceIdType.MESH
LENT = 96


def exchange(
    nx, ny, slots, vblocks, owned,
    work_in, row_in, col_in, feat_in, vals_ref,
    prod_ref, moved_ref, table_ref,
    vbuf0, vbuf1, stage, recv, fbuf, mbuf, live_ref, links, slinks, prefix,
    psend, precv, asend, arecv, qsend, qrecv, carried, ssend, srecv,
    work_ref, row_ref, col_ref, ready, xready,
    lsem, isem, insem, ms, mr, fs, fr, ts, tr, ps, pr, xs, xr, qs, qr, cs, cr,
):
    share = slots // ny
    half = ny // 2
    nh = ny // 2
    near_heights = nh // 2
    order = feat_in.shape[1]
    gx, gy = lax.axis_index("gx"), lax.axis_index("gy")
    side, height = lax.rem(gy, 2), gy // 2
    upper, place_in_half = gy // half, lax.rem(gy, half)
    base = upper * half

    held = (vbuf0, vbuf1)
    piece = slots // len(held)
    loads = [
        pltpu.make_async_copy(vals_ref.at[pl.ds(i * piece, piece)], ref, lsem.at[i])
        for i, ref in enumerate(held)
    ]
    fetches = [
        pltpu.make_async_copy(src, dst, insem.at[i])
        for i, (src, dst) in enumerate((
            (work_in, work_ref), (row_in, row_ref), (col_in, col_ref),
            (feat_in, fbuf.at[pl.ds(0, vblocks)]),
        ))
    ]
    for copy in fetches:
        copy.start()
    for copy in loads:
        copy.start()

    def near(d):
        return base + lax.rem(place_in_half + d, half)

    def around(d):
        return lax.rem(gy + d, ny)

    def along_x(d):
        return lax.rem(gx + d, nx)

    def remote(src, dst, send, arrive, where):
        return pltpu.make_async_remote_copy(
            src_ref=src, dst_ref=dst, send_sem=send, recv_sem=arrive,
            device_id=where, device_id_type=MESH,
        )

    def landed(ref, sem):
        pltpu.make_async_copy(ref, ref, sem).wait()

    def signal(sem, where):
        pl.semaphore_signal(sem, inc=1, device_id=where, device_id_type=MESH)

    def rank(c):
        return (c // 2 + lax.rem(c, 2)) * ny + c

    mine = rank(gy)

    def above(e):
        return rank(e) > mine

    def below(e):
        return rank(e) < mine

    lower = gx
    for d in range(1, ny):
        lower = lower + jnp.where(below(around(d)), 1, 0)
    barrier = pltpu.get_barrier_semaphore()
    for d in range(1, ny):
        pl.when(above(around(d)))(functools.partial(signal, barrier, (gx, around(d))))
    for d in range(1, nx):
        pl.when(along_x(d) > gx)(functools.partial(signal, barrier, (along_x(d), gy)))
    mbuf[gy] = jnp.zeros(mbuf.shape[1:], jnp.int32)
    recv[slots] = jnp.zeros(recv.shape[1:], recv.dtype)
    pl.when(lower > 0)(lambda: pl.semaphore_wait(barrier, lower))
    for d in range(1, ny):
        pl.when(below(around(d)))(functools.partial(signal, ready.at[gy], (gx, around(d))))
    for d in range(1, nx):
        pl.when(along_x(d) < gx)(functools.partial(signal, xready.at[gx], (along_x(d), gy)))
    for copy in fetches[:3]:
        copy.wait()
    for i, ref in enumerate((work_ref, row_ref, col_ref)):
        mbuf[gy, i : i + 1, 0:slots] = ref[...].reshape(1, slots)

    def answered(e):
        pl.when(above(e))(lambda: pl.semaphore_wait(ready.at[e], 1))

    def meta(c, e, i):
        return remote(mbuf.at[c], mbuf.at[c], ms, mr.at[i], (gx, e))

    metas = [meta(gy, near(d), d) for d in range(1, half)]
    for d in range(half - 1, 0, -1):
        pl.when(below(near(d)))(metas[d - 1].start)
    fetches[3].wait()
    feats = [
        remote(
            fbuf.at[pl.ds(0, vblocks)], fbuf.at[pl.ds(d * vblocks, vblocks)], fs, fr,
            (along_x(d), gy),
        )
        for d in range(1, nx)
    ]
    for d in range(1, nx):
        pl.when(along_x(d) < gx)(feats[d - 1].start)
    for d in range(1, half):
        answered(near(d))
        pl.when(above(near(d)))(metas[d - 1].start)

    at_end = (gy == 0) | (upper > 0)

    def share_features(now):
        for d in range(1, nx):
            @pl.when(now & (along_x(d) > gx))
            def _(d=d):
                pl.semaphore_wait(xready.at[along_x(d)], 1)
                feats[d - 1].start()

    share_features(~at_end)

    def needed(c):
        return jnp.where(upper > 0, c > gy, c < gy)

    def alive(c):
        return (mbuf[c, 0:1, :] > 0).astype(jnp.int32)

    live_ref[...] = alive(gy) * jnp.where(upper > 0, 1, 0)
    for d in range(1, half):
        @pl.when(needed(near(half - d)))
        def _(c=near(half - d), d=d):
            meta(c, c, d).wait_recv()
            live_ref[...] += alive(c)
    passed = jnp.sum(live_ref[...])
    start = lax.rem(jnp.where(upper > 0, ny * owned - passed, passed), ny)

    loads[0].wait()
    def target(across, up, over):
        h = (1 - upper if across else upper) * near_heights + lax.rem(
            lax.rem(height, near_heights) + up, near_heights
        )
        return h * 2 + (1 - side if over else side)

    def tile_at(k, shift):
        return held[k * ny // piece][k * ny % piece + shift]

    def send_tiles(across, up, over, low=0, high=share):
        e = target(across, up, over)
        if across and low == 0:
            answered(e)
        if (across, up, over, low) == (1, 0, 0, 0):
            meta(gy, e, 0).start()
        i = (across * near_heights + up) * 2 + over
        shift = lax.rem(e + ny - start, ny)
        for k in range(low, high):
            stage[i * share + k] = tile_at(k, shift)
        remote(
            stage.at[pl.ds(i * share + low, high - low)],
            recv.at[pl.ds(gy * share + low, high - low)],
            ts, tr, (gx, e),
        ).start()

    def cut(ways, low, high):
        return [(*way, low, high) for way in ways]

    mate = target(1, 0, 0)
    near_line = [(0, u, 0) for u in range(1, near_heights)]
    near_cross = [(0, u, 1) for u in range(1, near_heights)]
    far_line = [(1, u, 0) for u in range(near_heights)]
    far_cross = [(1, u, 1) for u in range(near_heights)]
    pair = [(0, 0, 1)]
    middle = near_heights // 2
    batches = [far_line[:middle] + near_line + pair + far_line[middle:], far_cross[:middle], near_cross + far_cross[middle:], []]
    send_tiles(*batches[0][0], 0, share // 2)
    loads[1].wait()
    send_tiles(*batches[0][0], share // 2, share)
    for way in batches[0][1:]:
        send_tiles(*way)
    share_features(at_end)
    shift = lax.rem(gy + ny - start, ny)
    for k in range(share):
        recv[gy * share + k] = tile_at(k, shift)

    prefix[slots] = jnp.zeros(prefix.shape[1:], jnp.float32)
    down = lax.broadcasted_iota(jnp.int32, (128, 128), 0)
    across = lax.broadcasted_iota(jnp.int32, (128, 128), 1)
    rows = jnp.where(across < slots, mbuf[gy, 1:2, :] - gx * (ny * vblocks), -1)
    upright = jnp.sum(jnp.where(down == across, rows, 0), axis=1, keepdims=True)
    prev = jnp.max(
        jnp.where((upright == rows) & (down < across), down, -1), axis=0, keepdims=True
    )
    last = jnp.max(jnp.where(upright == across, down, -1), axis=0, keepdims=True)
    links[...] = jnp.zeros((8, 128), jnp.int32)
    links[0:1, :] = jnp.where(prev < 0, slots, prev)
    links[1:2, :] = jnp.where(last < 0, slots, last)
    links[2:3, :] = mbuf[gy, 0:1, :]
    links[3:4, :] = mbuf[gy, 2:3, :]
    listing = pltpu.make_async_copy(links, slinks, isem)
    listing.start()
    listing.wait()
    landed(fbuf.at[pl.ds(vblocks, (nx - 1) * vblocks)], fr)
    pattern = lax.broadcasted_iota(jnp.int32, (order, order), 0) * order + lax.broadcasted_iota(
        jnp.int32, (order, order), 1
    )
    group = 4

    def multiply(i, step, carry):
        terms = []
        for u in range(group):
            t = i * piece + step * group + u
            values = held[i][step * group + u].astype(jnp.float32)
            masked = jnp.where(pattern < slinks[2, t], values, 0.0).astype(jnp.bfloat16)
            col = slinks[3, t]
            back = lax.rem(gx - col // vblocks // ny + nx, nx)
            block = fbuf[back * vblocks + lax.rem(col, vblocks)]
            terms.append(jnp.dot(masked, block, preferred_element_type=jnp.float32))
        for u in range(group):
            t = i * piece + step * group + u
            prefix[t] = terms[u] + prefix[slinks[0, t]]
        return carry

    for i in range(len(held)):
        lax.fori_loop(0, piece // group, functools.partial(multiply, i), 0)

    meta(mate, mate, 0).wait_recv()
    for d in range(1, half):
        remote(mbuf.at[mate], mbuf.at[mate], ms, mr.at[half], (gx, near(d))).start()

    def summed(h, q, v):
        return prefix[slinks[1, (h * 2 + q) * vblocks + v]]

    def beside(u):
        return upper * near_heights + lax.rem(lax.rem(height, near_heights) + u, near_heights)

    def heights(u):
        h = beside(u)
        return (h, nh - 1 - h)

    span = 2 * vblocks
    halves = {}
    for u in [*range(1, near_heights), 0]:
        for w, h in enumerate(heights(u)):
            for v in range(vblocks):
                psend[u * span + w * vblocks + v] = summed(h, 1 - side, v)
        where = pl.ds(u * span, span)
        copy = remote(
            psend.at[where], precv.at[where], ps, pr.at[u], (gx, gy + 1 - 2 * side)
        )
        copy.start()
        halves[u] = copy
    for way in batches[1]:
        send_tiles(*way)

    joins = []
    for u in range(1, near_heights):
        halves[u].wait_recv()
        for w, h in enumerate(heights(u)):
            for v in range(vblocks):
                at = u * span + w * vblocks + v
                asend[at] = summed(h, side, v) + precv[at]
        where = pl.ds(u * span, span)
        copy = remote(
            asend.at[where], arecv.at[where], xs, xr, (gx, beside(u) * 2 + side)
        )
        copy.start()
        joins.append(copy)
    for way in batches[2]:
        send_tiles(*way)

    halves[0].wait_recv()
    if joins:
        landed(arecv.at[pl.ds(span, len(joins) * span)], xr)

    def gathered(w, h, v):
        total = summed(h, side, v) + precv[w * vblocks + v]
        for u in range(1, near_heights):
            total = total + arecv[u * span + w * vblocks + v]
        return total

    mirror = nh - 1 - height
    for v in range(vblocks):
        term = gathered(1, mirror, v)
        peak = jnp.max(jnp.abs(term), axis=0, keepdims=True)
        small = peak < 2.0**-62
        term, peak = term * jnp.where(small, 2.0**64, 1.0), peak * jnp.where(small, 2.0**64, 1.0)
        term = term * jnp.where(peak > 0, 32767.0 / jnp.where(peak > 0, peak, 1.0), 0.0)
        term = (term + jnp.where(term < 0, -0.5, 0.5)).astype(jnp.int32)
        qsend[pl.ds(v * order, order)] = term.astype(jnp.int16)
        ssend[v : v + 1, :] = peak * (1.0 / 32767.0)
        ssend[vblocks + v : vblocks + v + 1, :] = jnp.where(small, 2.0**-64, 1.0)
    owner = (gx, mirror * 2 + side)
    tail = order * LENT // 128
    body, end = pl.ds(0, vblocks * order - tail), pl.ds(vblocks * order - tail, tail)
    lends, carries = (upper > 0) & (side == 0), (upper > 0) & (side == 1)
    partials = [
        remote(ssend, srecv, qs.at[0], qr.at[0], owner),
        remote(qsend.at[body], qrecv.at[body], qs.at[1], qr.at[1], owner),
    ]
    direct = remote(qsend.at[end], qrecv.at[end], qs.at[2], qr.at[2], owner)
    lent = remote(qsend.at[end], carried, qs.at[2], cr, (gx, lax.rem(gy + 1, ny)))
    carry_on = remote(carried, qrecv.at[end], cs, qr.at[2], (gx, lax.rem(mirror * 2 + 1 - side, ny)))
    pl.when(lends)(lent.start)

    @pl.when(carries)
    def _():
        lent.wait_recv()
        carry_on.start()

    for copy in partials:
        copy.start()
    pl.when(~lends)(direct.start)
    for way in batches[3]:
        send_tiles(*way)


    own = [gathered(0, height, v) for v in range(vblocks)]
    for d in range(1, half):
        c = near(half - d)
        pl.when(~needed(c))(meta(c, c, d).wait_recv)
    landed(mbuf.at[pl.ds(0, half - 1)], mr.at[half])
    count = [jnp.sum((mbuf[c, 0:1, :] > 0).astype(jnp.int32)) for c in range(ny)]
    first = [jnp.int32(0)]
    for c in range(ny - 1):
        first.append(first[-1] + count[c])
    table_ref[...] = jnp.zeros(table_ref.shape, jnp.int32)
    slot = lax.broadcasted_iota(jnp.int32, (1, 128), 1)
    wanted = slot * ny + gy
    at = jnp.full((1, 128), slots, jnp.int32)
    for c in range(ny):
        offset = c * share + (gy - first[c] + slots * ny) // ny - slots
        here = (wanted >= first[c]) & (wanted < first[c] + count[c])
        at = jnp.where(here, slot + offset, at)
    links[0:1, :] = at
    placing = pltpu.make_async_copy(links, slinks, isem)
    placing.start()
    lane = lax.broadcasted_iota(jnp.int32, (owned, 128), 1)
    line = lax.broadcasted_iota(jnp.int32, (owned, 128), 0)
    wanted = line * ny + gy
    sums = [jnp.zeros((owned, 128), jnp.int32) for _ in range(3)]
    for c in range(ny):
        work = mbuf[c, 0:1, :]
        hit = (lane + first[c] == wanted) & (work > 0)
        for i in range(3):
            sums[i] = sums[i] + jnp.where(hit, mbuf[c, i : i + 1, :], 0)
    for i in range(3):
        column = jnp.sum(sums[i], axis=1, keepdims=True)
        spread = jnp.where(line == lane, jnp.broadcast_to(column, (owned, 128)), 0)
        table_ref[i : i + 1, :] = jnp.sum(spread, axis=0, keepdims=True)

    placing.wait()
    landed(recv.at[pl.ds(0, (ny - 1) * share)], tr)

    def settle(s, carry):
        moved_ref[s] = recv[slinks[0, s]]
        return carry

    lax.fori_loop(0, owned, settle, 0, unroll=4)
    for copy in (*partials, direct):
        copy.wait_recv()
    for v in range(vblocks):
        coded = qrecv[pl.ds(v * order, order)].astype(jnp.int32).astype(jnp.float32)
        scale = srecv[v : v + 1, :]
        prod_ref[v] = own[v] + coded * scale * srecv[vblocks + v : vblocks + v + 1, :]
    landed(mbuf.at[pl.ds(0, ny - 1)], ms)
    landed(fbuf.at[pl.ds(0, (nx - 1) * vblocks)], fs)
    landed(stage.at[pl.ds(0, (ny - 1) * share)], ts)
    landed(psend, ps)
    if joins:
        landed(asend.at[pl.ds(span, len(joins) * span)], xs)
    for copy in (*partials, direct):
        copy.wait_send()
    pl.when(carries)(carry_on.wait_send)


def deliver(owned, meta_ref, prod_ref, moved_ref, prod_out, moved_out, row_out, col_out, work_out, lists, sems):
    part = owned // 1
    outs = [(prod_ref, prod_out)]
    for i in range(1):
        where = pl.ds(i * part, part)
        outs.append((moved_ref.at[where], moved_out.at[where]))
    for i, ref in enumerate((work_out, row_out, col_out)):
        lists[i] = meta_ref[i, 0:owned]
        outs.append((lists.at[i], ref))
    copies = [pltpu.make_async_copy(*pair, sems.at[i]) for i, pair in enumerate(outs)]
    for copy in copies:
        copy.start()
    for copy in copies:
        copy.wait()


def size(shape, kind):
    total = jnp.dtype(kind).itemsize
    for extent in shape:
        total *= extent
    return total


def on_device(nx, ny, features, tile_vals, tile_row, tile_col, tile_work):
    slots, order = tile_vals.shape[:2]
    width = features.shape[1]
    vblocks = features.shape[0] // order
    owned = slots // 2
    near_heights = ny // 4
    half_blocks = near_heights * 2 * vblocks
    vmem = pl.BlockSpec(memory_space=pltpu.VMEM)
    anywhere = pl.BlockSpec(memory_space=pl.ANY)
    hbm = pl.BlockSpec(memory_space=pltpu.HBM)
    bf, f32, i32 = jnp.bfloat16, jnp.float32, jnp.int32
    dma = pltpu.SemaphoreType.DMA
    buffers = [
        ((slots // 2, order, order), bf),
        ((slots // 2, order, order), bf),
        ((slots, order, order), bf),
        ((slots + 1, order, order), bf),
        ((nx * vblocks, order, width), bf),
        ((ny, 4, 128), i32),
        ((1, 128), i32),
        ((8, 128), i32),
        None,
        ((slots + 1, order, width), f32),
        ((half_blocks, order, width), f32),
        ((half_blocks, order, width), f32),
        ((half_blocks, order, width), f32),
        ((half_blocks, order, width), f32),
        ((vblocks * order, width), jnp.int16),
        ((vblocks * order, width), jnp.int16),
        ((order * LENT // 128, width), jnp.int16),
        ((2 * vblocks, width), f32),
        ((2 * vblocks, width), f32),
    ]
    results = (
        jax.ShapeDtypeStruct((vblocks, order, width), f32),
        jax.ShapeDtypeStruct((owned, order, order), bf),
        jax.ShapeDtypeStruct((8, 128), i32),
    )
    need = sum(size(*b) for b in buffers if b) + sum(size(r.shape, r.dtype) for r in results)
    product, moved, table = pl.pallas_call(
        functools.partial(exchange, nx, ny, slots, vblocks, owned),
        out_shape=results,
        in_specs=[hbm] * 5,
        out_specs=(vmem, vmem, vmem),
        scratch_shapes=[
            pltpu.VMEM(*b) if b else pltpu.SMEM((8, 128), i32) for b in buffers
        ] + [
            pltpu.VMEM((slots,), i32),
            pltpu.VMEM((slots,), i32),
            pltpu.VMEM((slots,), i32),
            pltpu.SemaphoreType.REGULAR((ny,)), pltpu.SemaphoreType.REGULAR((nx,)),
            dma((2,)), dma, dma((4,)), dma, dma((ny // 2 + 1,)), dma, dma,
            dma, dma, dma, dma((near_heights,)), dma, dma, dma((3,)), dma((3,)), dma, dma,
        ],
        compiler_params=pltpu.CompilerParams(
            collective_id=0, has_side_effects=True, vmem_limit_bytes=need + 4 * 2**20
        ),
    )(*(
        pltpu.with_memory_space_constraint(x, pltpu.HBM)
        for x in (
            tile_work, tile_row, tile_col,
            features.reshape(vblocks, order, width), tile_vals,
        )
    ))
    index = jax.ShapeDtypeStruct((owned,), i32)
    product, moved, row, col, work = pl.pallas_call(
        functools.partial(deliver, owned),
        out_shape=(
            jax.ShapeDtypeStruct((vblocks, order, width), f32),
            jax.ShapeDtypeStruct((owned, order, order), bf),
            index, index, index,
        ),
        in_specs=[vmem, vmem, vmem],
        out_specs=(hbm,) * 5,
        scratch_shapes=[pltpu.VMEM((3, owned), i32), dma((4 + 1,))],
        compiler_params=pltpu.CompilerParams(vmem_limit_bytes=4 * 2**20),
    )(table, product, moved)
    return product.reshape(vblocks * order, width), moved, row, col, work


def solution(mesh):
    both = ("gx", "gy")
    return jax.shard_map(
        functools.partial(on_device, mesh.shape["gx"], mesh.shape["gy"]),
        mesh=mesh,
        in_specs=(P(both, None), P(both, None, None), P(both), P(both), P(both)),
        out_specs=(P(both, None), P(both, None, None), P(both), P(both), P(both)),
        check_vma=False,
    )
```

```python
import functools

import jax
import jax.numpy as jnp
from jax import lax
from jax.experimental import pallas as pl
from jax.experimental.pallas import tpu as pltpu
from jax.sharding import PartitionSpec as P

MESH = pl.DeviceIdType.MESH
LENT = 96


def exchange(
    nx, ny, slots, vblocks, owned,
    work_in, row_in, col_in, feat_in, vals_ref,
    prod_ref, moved_ref, table_ref,
    vbuf0, vbuf1, stage, recv, fbuf, mbuf, live_ref, links, slinks, prefix,
    psend, precv, asend, arecv, qsend, qrecv, carried, ssend, srecv,
    work_ref, row_ref, col_ref, ready, xready,
    lsem, isem, insem, ms, mr, fs, fr, ts, tr, ps, pr, xs, xr, qs, qr, cs, cr,
):
    share = slots // ny
    half = ny // 2
    nh = ny // 2
    near_heights = nh // 2
    order = feat_in.shape[1]
    gx, gy = lax.axis_index("gx"), lax.axis_index("gy")
    side, height = lax.rem(gy, 2), gy // 2
    upper, place_in_half = gy // half, lax.rem(gy, half)
    base = upper * half

    held = (vbuf0, vbuf1)
    piece = slots // len(held)
    loads = [
        pltpu.make_async_copy(vals_ref.at[pl.ds(i * piece, piece)], ref, lsem.at[i])
        for i, ref in enumerate(held)
    ]
    fetches = [
        pltpu.make_async_copy(src, dst, insem.at[i])
        for i, (src, dst) in enumerate((
            (work_in, work_ref), (row_in, row_ref), (col_in, col_ref),
            (feat_in, fbuf.at[pl.ds(0, vblocks)]),
        ))
    ]
    for copy in fetches:
        copy.start()
    for copy in loads:
        copy.start()

    def near(d):
        return base + lax.rem(place_in_half + d, half)

    def around(d):
        return lax.rem(gy + d, ny)

    def along_x(d):
        return lax.rem(gx + d, nx)

    def remote(src, dst, send, arrive, where):
        return pltpu.make_async_remote_copy(
            src_ref=src, dst_ref=dst, send_sem=send, recv_sem=arrive,
            device_id=where, device_id_type=MESH,
        )

    def landed(ref, sem):
        pltpu.make_async_copy(ref, ref, sem).wait()

    def signal(sem, where):
        pl.semaphore_signal(sem, inc=1, device_id=where, device_id_type=MESH)

    def rank(c):
        return (c // 2 + lax.rem(c, 2)) * ny + c

    mine = rank(gy)

    def above(e):
        return rank(e) > mine

    def below(e):
        return rank(e) < mine

    lower = gx
    for d in range(1, ny):
        lower = lower + jnp.where(below(around(d)), 1, 0)
    barrier = pltpu.get_barrier_semaphore()
    for d in range(1, ny):
        pl.when(above(around(d)))(functools.partial(signal, barrier, (gx, around(d))))
    for d in range(1, nx):
        pl.when(along_x(d) > gx)(functools.partial(signal, barrier, (along_x(d), gy)))
    mbuf[gy] = jnp.zeros(mbuf.shape[1:], jnp.int32)
    recv[slots] = jnp.zeros(recv.shape[1:], recv.dtype)
    pl.when(lower > 0)(lambda: pl.semaphore_wait(barrier, lower))
    for d in range(1, ny):
        pl.when(below(around(d)))(functools.partial(signal, ready.at[gy], (gx, around(d))))
    for d in range(1, nx):
        pl.when(along_x(d) < gx)(functools.partial(signal, xready.at[gx], (along_x(d), gy)))
    for copy in fetches[:3]:
        copy.wait()
    for i, ref in enumerate((work_ref, row_ref, col_ref)):
        mbuf[gy, i : i + 1, 0:slots] = ref[...].reshape(1, slots)

    def answered(e):
        pl.when(above(e))(lambda: pl.semaphore_wait(ready.at[e], 1))

    def meta(c, e, i):
        return remote(mbuf.at[c], mbuf.at[c], ms, mr.at[i], (gx, e))

    metas = [meta(gy, near(d), d) for d in range(1, half)]
    for d in range(half - 1, 0, -1):
        pl.when(below(near(d)))(metas[d - 1].start)
    fetches[3].wait()
    feats = [
        remote(
            fbuf.at[pl.ds(0, vblocks)], fbuf.at[pl.ds(d * vblocks, vblocks)], fs, fr,
            (along_x(d), gy),
        )
        for d in range(1, nx)
    ]
    for d in range(1, nx):
        pl.when(along_x(d) < gx)(feats[d - 1].start)
    for d in range(1, half):
        answered(near(d))
        pl.when(above(near(d)))(metas[d - 1].start)

    at_end = (gy == 0) | (upper > 0)

    def share_features(now):
        for d in range(1, nx):
            @pl.when(now & (along_x(d) > gx))
            def _(d=d):
                pl.semaphore_wait(xready.at[along_x(d)], 1)
                feats[d - 1].start()

    share_features(~at_end)

    def needed(c):
        return jnp.where(upper > 0, c > gy, c < gy)

    def alive(c):
        return (mbuf[c, 0:1, :] > 0).astype(jnp.int32)

    live_ref[...] = alive(gy) * jnp.where(upper > 0, 1, 0)
    for d in range(1, half):
        @pl.when(needed(near(half - d)))
        def _(c=near(half - d), d=d):
            meta(c, c, d).wait_recv()
            live_ref[...] += alive(c)
    passed = jnp.sum(live_ref[...])
    start = lax.rem(jnp.where(upper > 0, ny * owned - passed, passed), ny)

    loads[0].wait()

    def target(across, up, over):
        h = (1 - upper if across else upper) * near_heights + lax.rem(
            lax.rem(height, near_heights) + up, near_heights
        )
        return h * 2 + (1 - side if over else side)

    def tile_at(k, shift):
        return held[k * ny // piece][k * ny % piece + shift]

    def send_tiles(across, up, over, low=0, high=share):
        e = target(across, up, over)
        if across and low == 0:
            answered(e)
        if (across, up, over, low) == (1, 0, 0, 0):
            meta(gy, e, 0).start()
        i = (across * near_heights + up) * 2 + over
        shift = lax.rem(e + ny - start, ny)
        for k in range(low, high):
            stage[i * share + k] = tile_at(k, shift)
        remote(
            stage.at[pl.ds(i * share + low, high - low)],
            recv.at[pl.ds(gy * share + low, high - low)],
            ts, tr, (gx, e),
        ).start()

    mate = target(1, 0, 0)
    near_line = [(0, u, 0) for u in range(1, near_heights)]
    near_cross = [(0, u, 1) for u in range(1, near_heights)]
    far_line = [(1, u, 0) for u in range(near_heights)]
    far_cross = [(1, u, 1) for u in range(near_heights)]
    pair = [(0, 0, 1)]
    middle = near_heights // 2
    batches = [
        far_line[:middle] + pair + far_line[middle:] + near_line,
        far_cross[:middle],
        near_cross + far_cross[middle:],
    ]
    send_tiles(*batches[0][0], 0, share // 2)
    loads[1].wait()
    send_tiles(*batches[0][0], share // 2, share)
    for way in batches[0][1:]:
        send_tiles(*way)
    share_features(at_end)
    shift = lax.rem(gy + ny - start, ny)
    for k in range(share):
        recv[gy * share + k] = tile_at(k, shift)

    prefix[slots] = jnp.zeros(prefix.shape[1:], jnp.float32)
    down = lax.broadcasted_iota(jnp.int32, (128, 128), 0)
    across = lax.broadcasted_iota(jnp.int32, (128, 128), 1)
    rows = jnp.where(across < slots, mbuf[gy, 1:2, :] - gx * (ny * vblocks), -1)
    upright = jnp.sum(jnp.where(down == across, rows, 0), axis=1, keepdims=True)
    prev = jnp.max(
        jnp.where((upright == rows) & (down < across), down, -1), axis=0, keepdims=True
    )
    last = jnp.max(jnp.where(upright == across, down, -1), axis=0, keepdims=True)
    links[...] = jnp.zeros((8, 128), jnp.int32)
    links[0:1, :] = jnp.where(prev < 0, slots, prev)
    links[1:2, :] = jnp.where(last < 0, slots, last)
    links[2:3, :] = mbuf[gy, 0:1, :]
    links[3:4, :] = mbuf[gy, 2:3, :]
    listing = pltpu.make_async_copy(links, slinks, isem)
    listing.start()
    listing.wait()
    landed(fbuf.at[pl.ds(vblocks, (nx - 1) * vblocks)], fr)
    pattern = lax.broadcasted_iota(jnp.int32, (order, order), 0) * order + lax.broadcasted_iota(
        jnp.int32, (order, order), 1
    )
    group = 4

    def multiply(i, step, carry):
        terms = []
        for u in range(group):
            t = i * piece + step * group + u
            values = held[i][step * group + u].astype(jnp.float32)
            masked = jnp.where(pattern < slinks[2, t], values, 0.0).astype(jnp.bfloat16)
            col = slinks[3, t]
            back = lax.rem(gx - col // vblocks // ny + nx, nx)
            block = fbuf[back * vblocks + lax.rem(col, vblocks)]
            terms.append(jnp.dot(masked, block, preferred_element_type=jnp.float32))
        for u in range(group):
            t = i * piece + step * group + u
            prefix[t] = terms[u] + prefix[slinks[0, t]]
        return carry

    for i in range(len(held)):
        lax.fori_loop(0, piece // group, functools.partial(multiply, i), 0)

    meta(mate, mate, 0).wait_recv()
    for d in range(1, half):
        remote(mbuf.at[mate], mbuf.at[mate], ms, mr.at[half], (gx, near(d))).start()

    def summed(h, q, v):
        return prefix[slinks[1, (h * 2 + q) * vblocks + v]]

    def beside(u):
        return upper * near_heights + lax.rem(lax.rem(height, near_heights) + u, near_heights)

    def heights(u):
        h = beside(u)
        return (h, nh - 1 - h)

    span = 2 * vblocks
    halves = {}
    for u in [*range(1, near_heights), 0]:
        for w, h in enumerate(heights(u)):
            for v in range(vblocks):
                psend[u * span + w * vblocks + v] = summed(h, 1 - side, v)
        where = pl.ds(u * span, span)
        copy = remote(
            psend.at[where], precv.at[where], ps, pr.at[u], (gx, gy + 1 - 2 * side)
        )
        copy.start()
        halves[u] = copy
    for way in batches[1]:
        send_tiles(*way)

    joins = []
    for u in range(1, near_heights):
        halves[u].wait_recv()
        for w, h in enumerate(heights(u)):
            for v in range(vblocks):
                at = u * span + w * vblocks + v
                asend[at] = summed(h, side, v) + precv[at]
        where = pl.ds(u * span, span)
        copy = remote(
            asend.at[where], arecv.at[where], xs, xr, (gx, beside(u) * 2 + side)
        )
        copy.start()
        joins.append(copy)
    for way in batches[2]:
        send_tiles(*way)

    halves[0].wait_recv()
    if joins:
        landed(arecv.at[pl.ds(span, len(joins) * span)], xr)

    def gathered(w, h, v):
        total = summed(h, side, v) + precv[w * vblocks + v]
        for u in range(1, near_heights):
            total = total + arecv[u * span + w * vblocks + v]
        return total

    mirror = nh - 1 - height
    for v in range(vblocks):
        term = gathered(1, mirror, v)
        peak = jnp.max(jnp.abs(term), axis=0, keepdims=True)
        small = peak < 2.0**-62
        term, peak = term * jnp.where(small, 2.0**64, 1.0), peak * jnp.where(small, 2.0**64, 1.0)
        term = term * jnp.where(peak > 0, 32767.0 / jnp.where(peak > 0, peak, 1.0), 0.0)
        term = (term + jnp.where(term < 0, -0.5, 0.5)).astype(jnp.int32)
        qsend[pl.ds(v * order, order)] = term.astype(jnp.int16)
        ssend[v : v + 1, :] = peak * (1.0 / 32767.0)
        ssend[vblocks + v : vblocks + v + 1, :] = jnp.where(small, 2.0**-64, 1.0)
    owner = (gx, mirror * 2 + side)
    tail = order * LENT // 128
    body, end = pl.ds(0, vblocks * order - tail), pl.ds(vblocks * order - tail, tail)
    lends, carries = (upper > 0) & (side == 0), (upper > 0) & (side == 1)
    partials = [
        remote(ssend, srecv, qs.at[0], qr.at[0], owner),
        remote(qsend.at[body], qrecv.at[body], qs.at[1], qr.at[1], owner),
    ]
    direct = remote(qsend.at[end], qrecv.at[end], qs.at[2], qr.at[2], owner)
    lent = remote(qsend.at[end], carried, qs.at[2], cr, (gx, lax.rem(gy + 1, ny)))
    carry_on = remote(carried, qrecv.at[end], cs, qr.at[2], (gx, lax.rem(mirror * 2 + 1 - side, ny)))
    pl.when(lends)(lent.start)

    @pl.when(carries)
    def _():
        lent.wait_recv()
        carry_on.start()

    for copy in partials:
        copy.start()
    pl.when(~lends)(direct.start)

    own = [gathered(0, height, v) for v in range(vblocks)]
    for d in range(1, half):
        c = near(half - d)
        pl.when(~needed(c))(meta(c, c, d).wait_recv)
    landed(mbuf.at[pl.ds(0, half - 1)], mr.at[half])
    count = [jnp.sum((mbuf[c, 0:1, :] > 0).astype(jnp.int32)) for c in range(ny)]
    first = [jnp.int32(0)]
    for c in range(ny - 1):
        first.append(first[-1] + count[c])
    table_ref[...] = jnp.zeros(table_ref.shape, jnp.int32)
    slot = lax.broadcasted_iota(jnp.int32, (1, 128), 1)
    wanted = slot * ny + gy
    at = jnp.full((1, 128), slots, jnp.int32)
    for c in range(ny):
        offset = c * share + (gy - first[c] + slots * ny) // ny - slots
        here = (wanted >= first[c]) & (wanted < first[c] + count[c])
        at = jnp.where(here, slot + offset, at)
    links[0:1, :] = at
    placing = pltpu.make_async_copy(links, slinks, isem)
    placing.start()
    lane = lax.broadcasted_iota(jnp.int32, (owned, 128), 1)
    line = lax.broadcasted_iota(jnp.int32, (owned, 128), 0)
    wanted = line * ny + gy
    sums = [jnp.zeros((owned, 128), jnp.int32) for _ in range(3)]
    for c in range(ny):
        work = mbuf[c, 0:1, :]
        hit = (lane + first[c] == wanted) & (work > 0)
        for i in range(3):
            sums[i] = sums[i] + jnp.where(hit, mbuf[c, i : i + 1, :], 0)
    for i in range(3):
        column = jnp.sum(sums[i], axis=1, keepdims=True)
        spread = jnp.where(line == lane, jnp.broadcast_to(column, (owned, 128)), 0)
        table_ref[i : i + 1, :] = jnp.sum(spread, axis=0, keepdims=True)

    placing.wait()
    landed(recv.at[pl.ds(0, (ny - 1) * share)], tr)

    def settle(s, carry):
        moved_ref[s] = recv[slinks[0, s]]
        return carry

    lax.fori_loop(0, owned, settle, 0, unroll=4)
    for copy in (*partials, direct):
        copy.wait_recv()
    for v in range(vblocks):
        coded = qrecv[pl.ds(v * order, order)].astype(jnp.int32).astype(jnp.float32)
        scale = srecv[v : v + 1, :]
        prod_ref[v] = own[v] + coded * scale * srecv[vblocks + v : vblocks + v + 1, :]
    landed(mbuf.at[pl.ds(0, ny - 1)], ms)
    landed(fbuf.at[pl.ds(0, (nx - 1) * vblocks)], fs)
    landed(stage.at[pl.ds(0, (ny - 1) * share)], ts)
    landed(psend, ps)
    if joins:
        landed(asend.at[pl.ds(span, len(joins) * span)], xs)
    for copy in (*partials, direct):
        copy.wait_send()
    pl.when(carries)(carry_on.wait_send)


def deliver(owned, meta_ref, prod_ref, moved_ref, prod_out, moved_out, row_out, col_out, work_out, lists, sems):
    copies = [
        pltpu.make_async_copy(moved_ref, moved_out, sems.at[0]),
        pltpu.make_async_copy(prod_ref, prod_out, sems.at[1]),
    ]
    for copy in copies:
        copy.start()
    for i, ref in enumerate((work_out, row_out, col_out)):
        lists[i] = meta_ref[i, 0:owned]
        copies.append(pltpu.make_async_copy(lists.at[i], ref, sems.at[2 + i]))
        copies[-1].start()
    for copy in copies:
        copy.wait()


def size(shape, kind):
    total = jnp.dtype(kind).itemsize
    for extent in shape:
        total *= extent
    return total


def on_device(nx, ny, features, tile_vals, tile_row, tile_col, tile_work):
    slots, order = tile_vals.shape[:2]
    width = features.shape[1]
    vblocks = features.shape[0] // order
    owned = slots // 2
    near_heights = ny // 4
    half_blocks = near_heights * 2 * vblocks
    vmem = pl.BlockSpec(memory_space=pltpu.VMEM)
    hbm = pl.BlockSpec(memory_space=pltpu.HBM)
    bf, f32, i32 = jnp.bfloat16, jnp.float32, jnp.int32
    dma = pltpu.SemaphoreType.DMA
    buffers = [
        ((slots // 2, order, order), bf),
        ((slots // 2, order, order), bf),
        ((slots, order, order), bf),
        ((slots + 1, order, order), bf),
        ((nx * vblocks, order, width), bf),
        ((ny, 4, 128), i32),
        ((1, 128), i32),
        ((8, 128), i32),
        None,
        ((slots + 1, order, width), f32),
        ((half_blocks, order, width), f32),
        ((half_blocks, order, width), f32),
        ((half_blocks, order, width), f32),
        ((half_blocks, order, width), f32),
        ((vblocks * order, width), jnp.int16),
        ((vblocks * order, width), jnp.int16),
        ((order * LENT // 128, width), jnp.int16),
        ((2 * vblocks, width), f32),
        ((2 * vblocks, width), f32),
    ]
    results = (
        jax.ShapeDtypeStruct((vblocks, order, width), f32),
        jax.ShapeDtypeStruct((owned, order, order), bf),
        jax.ShapeDtypeStruct((8, 128), i32),
    )
    need = sum(size(*b) for b in buffers if b) + sum(size(r.shape, r.dtype) for r in results)
    product, moved, table = pl.pallas_call(
        functools.partial(exchange, nx, ny, slots, vblocks, owned),
        out_shape=results,
        in_specs=[hbm] * 5,
        out_specs=(vmem, vmem, vmem),
        scratch_shapes=[
            pltpu.VMEM(*b) if b else pltpu.SMEM((8, 128), i32) for b in buffers
        ] + [
            pltpu.VMEM((slots,), i32),
            pltpu.VMEM((slots,), i32),
            pltpu.VMEM((slots,), i32),
            pltpu.SemaphoreType.REGULAR((ny,)), pltpu.SemaphoreType.REGULAR((nx,)),
            dma((2,)), dma, dma((4,)), dma, dma((ny // 2 + 1,)), dma, dma,
            dma, dma, dma, dma((near_heights,)), dma, dma, dma((3,)), dma((3,)), dma, dma,
        ],
        compiler_params=pltpu.CompilerParams(
            collective_id=0, has_side_effects=True, vmem_limit_bytes=need + 4 * 2**20
        ),
    )(*(
        pltpu.with_memory_space_constraint(x, pltpu.HBM)
        for x in (
            tile_work, tile_row, tile_col,
            features.reshape(vblocks, order, width), tile_vals,
        )
    ))
    index = jax.ShapeDtypeStruct((owned,), i32)
    product, moved, row, col, work = pl.pallas_call(
        functools.partial(deliver, owned),
        out_shape=(
            jax.ShapeDtypeStruct((vblocks, order, width), f32),
            jax.ShapeDtypeStruct((owned, order, order), bf),
            index, index, index,
        ),
        in_specs=[vmem, vmem, vmem],
        out_specs=(hbm,) * 5,
        scratch_shapes=[pltpu.VMEM((3, owned), i32), dma((5,))],
        compiler_params=pltpu.CompilerParams(vmem_limit_bytes=4 * 2**20),
    )(table, product, moved)
    return product.reshape(vblocks * order, width), moved, row, col, work


def solution(mesh):
    both = ("gx", "gy")
    return jax.shard_map(
        functools.partial(on_device, mesh.shape["gx"], mesh.shape["gy"]),
        mesh=mesh,
        in_specs=(P(both, None), P(both, None, None), P(both), P(both), P(both)),
        out_specs=(P(both, None), P(both, None, None), P(both), P(both), P(both)),
        check_vma=False,
    )
```

```python
import functools

import jax
import jax.numpy as jnp
from jax import lax
from jax.experimental import pallas as pl
from jax.experimental.pallas import tpu as pltpu
from jax.sharding import PartitionSpec as P

MESH = pl.DeviceIdType.MESH
LENT = 96


def exchange(
    nx, ny, slots, vblocks, owned,
    work_in, row_in, col_in, feat_in, vals_ref,
    prod_ref, moved_ref, table_ref,
    vbuf0, vbuf1, stage, recv, fbuf, mbuf, live_ref, links, slinks, prefix,
    psend, precv, asend, arecv, qsend, qrecv, carried, ssend, srecv,
    work_ref, row_ref, col_ref, ready, xready,
    lsem, isem, insem, ms, mr, fs, fr, ts, tr, ps, pr, xr, qs, qr, cs, cr,
):
    share = slots // ny
    half = ny // 2
    nh = ny // 2
    near_heights = nh // 2
    order = feat_in.shape[1]
    gx, gy = lax.axis_index("gx"), lax.axis_index("gy")
    side, height = lax.rem(gy, 2), gy // 2
    upper, place_in_half = gy // half, lax.rem(gy, half)
    base = upper * half

    held = (vbuf0, vbuf1)
    piece = slots // len(held)
    loads = [
        pltpu.make_async_copy(vals_ref.at[pl.ds(i * piece, piece)], ref, lsem.at[i])
        for i, ref in enumerate(held)
    ]
    fetches = [
        pltpu.make_async_copy(src, dst, insem.at[i])
        for i, (src, dst) in enumerate((
            (work_in, work_ref), (row_in, row_ref), (col_in, col_ref),
            (feat_in, fbuf.at[pl.ds(0, vblocks)]),
        ))
    ]
    for copy in fetches:
        copy.start()
    for copy in loads:
        copy.start()

    def near(d):
        return base + lax.rem(place_in_half + d, half)

    def around(d):
        return lax.rem(gy + d, ny)

    def along_x(d):
        return lax.rem(gx + d, nx)

    def remote(src, dst, send, arrive, where):
        return pltpu.make_async_remote_copy(
            src_ref=src, dst_ref=dst, send_sem=send, recv_sem=arrive,
            device_id=where, device_id_type=MESH,
        )

    def landed(ref, sem):
        pltpu.make_async_copy(ref, ref, sem).wait()

    def signal(sem, where):
        pl.semaphore_signal(sem, inc=1, device_id=where, device_id_type=MESH)

    def rank(c):
        return (c // 2 + lax.rem(c, 2)) * ny + c

    mine = rank(gy)

    def above(e):
        return rank(e) > mine

    def below(e):
        return rank(e) < mine

    lower = gx
    for d in range(1, ny):
        lower = lower + jnp.where(below(around(d)), 1, 0)
    barrier = pltpu.get_barrier_semaphore()
    for d in range(1, ny):
        pl.when(above(around(d)))(functools.partial(signal, barrier, (gx, around(d))))
    for d in range(1, nx):
        pl.when(along_x(d) > gx)(functools.partial(signal, barrier, (along_x(d), gy)))
    mbuf[gy] = jnp.zeros(mbuf.shape[1:], jnp.int32)
    recv[slots] = jnp.zeros(recv.shape[1:], recv.dtype)
    pl.when(lower > 0)(lambda: pl.semaphore_wait(barrier, lower))
    for d in range(1, ny):
        pl.when(below(around(d)))(functools.partial(signal, ready.at[gy], (gx, around(d))))
    for d in range(1, nx):
        pl.when(along_x(d) < gx)(functools.partial(signal, xready, (along_x(d), gy)))
    for copy in fetches[:3]:
        copy.wait()
    for i, ref in enumerate((work_ref, row_ref, col_ref)):
        mbuf[gy, i : i + 1, 0:slots] = ref[...].reshape(1, slots)

    def answered(e):
        pl.when(above(e))(lambda: pl.semaphore_wait(ready.at[e], 1))

    def meta(c, e, i):
        return remote(mbuf.at[c], mbuf.at[c], ms, mr.at[i], (gx, e))

    metas = [meta(gy, near(d), d) for d in range(1, half)]
    for d in range(half - 1, 0, -1):
        pl.when(below(near(d)))(metas[d - 1].start)
    fetches[3].wait()
    feats = [
        remote(
            fbuf.at[pl.ds(0, vblocks)], fbuf.at[pl.ds(d * vblocks, vblocks)], fs, fr,
            (along_x(d), gy),
        )
        for d in range(1, nx)
    ]
    for d in range(1, nx):
        pl.when(along_x(d) < gx)(feats[d - 1].start)
    for d in range(1, half):
        answered(near(d))
        pl.when(above(near(d)))(metas[d - 1].start)

    at_end = (gy == 0) | (upper > 0)

    def share_features(now):
        pl.when(now & (gx < nx - 1))(lambda: pl.semaphore_wait(xready, nx - 1 - gx))
        for d in range(1, nx):
            pl.when(now & (along_x(d) > gx))(feats[d - 1].start)

    share_features(~at_end)

    def needed(c):
        return jnp.where(upper > 0, c > gy, c < gy)

    def alive(c):
        return (mbuf[c, 0:1, :] > 0).astype(jnp.int32)

    live_ref[...] = alive(gy) * jnp.where(upper > 0, 1, 0)
    for d in range(1, half):
        @pl.when(needed(near(half - d)))
        def _(c=near(half - d), d=d):
            meta(c, c, d).wait_recv()
            live_ref[...] += alive(c)
    passed = jnp.sum(live_ref[...])
    start = lax.rem(jnp.where(upper > 0, ny * owned - passed, passed), ny)

    loads[0].wait()
    def target(across, up, over):
        h = (1 - upper if across else upper) * near_heights + lax.rem(
            lax.rem(height, near_heights) + up, near_heights
        )
        return h * 2 + (1 - side if over else side)

    def tile_at(k, shift):
        return held[k * ny // piece][k * ny % piece + shift]

    def send_tiles(across, up, over, low=0, high=share):
        e = target(across, up, over)
        if across and low == 0:
            answered(e)
        if (across, up, over, low) == (1, 0, 0, 0):
            meta(gy, e, 0).start()
        i = (across * near_heights + up) * 2 + over
        shift = lax.rem(e + ny - start, ny)
        for k in range(low, high):
            stage[i * share + k] = tile_at(k, shift)
        remote(
            stage.at[pl.ds(i * share + low, high - low)],
            recv.at[pl.ds(gy * share + low, high - low)],
            ts, tr, (gx, e),
        ).start()

    def cut(ways, low, high):
        return [(*way, low, high) for way in ways]

    mate = target(1, 0, 0)
    near_line = [(0, u, 0) for u in range(1, near_heights)]
    near_cross = [(0, u, 1) for u in range(1, near_heights)]
    far_line = [(1, u, 0) for u in range(near_heights)]
    far_cross = [(1, u, 1) for u in range(near_heights)]
    pair = [(0, 0, 1)]
    middle = near_heights // 2
    batches = [far_line[:middle] + near_line + pair + far_line[middle:], far_cross[:middle], near_cross + far_cross[middle:], []]
    send_tiles(*batches[0][0], 0, share // 2)
    loads[1].wait()
    send_tiles(*batches[0][0], share // 2, share)
    for way in batches[0][1:]:
        send_tiles(*way)
    share_features(at_end)
    shift = lax.rem(gy + ny - start, ny)
    for k in range(share):
        recv[gy * share + k] = tile_at(k, shift)

    prefix[slots] = jnp.zeros(prefix.shape[1:], jnp.float32)
    down = lax.broadcasted_iota(jnp.int32, (128, 128), 0)
    across = lax.broadcasted_iota(jnp.int32, (128, 128), 1)
    rows = jnp.where(across < slots, mbuf[gy, 1:2, :] - gx * (ny * vblocks), -1)
    upright = jnp.sum(jnp.where(down == across, rows, 0), axis=1, keepdims=True)
    prev = jnp.max(
        jnp.where((upright == rows) & (down < across), down, -1), axis=0, keepdims=True
    )
    last = jnp.max(jnp.where(upright == across, down, -1), axis=0, keepdims=True)
    links[...] = jnp.zeros((8, 128), jnp.int32)
    links[0:1, :] = jnp.where(prev < 0, slots, prev)
    links[1:2, :] = jnp.where(last < 0, slots, last)
    links[2:3, :] = mbuf[gy, 0:1, :]
    links[3:4, :] = mbuf[gy, 2:3, :]
    listing = pltpu.make_async_copy(links, slinks, isem)
    listing.start()
    listing.wait()
    landed(fbuf.at[pl.ds(vblocks, (nx - 1) * vblocks)], fr)
    pattern = lax.broadcasted_iota(jnp.int32, (order, order), 0) * order + lax.broadcasted_iota(
        jnp.int32, (order, order), 1
    )
    group = 4

    def multiply(i, step, carry):
        terms = []
        for u in range(group):
            t = i * piece + step * group + u
            values = held[i][step * group + u].astype(jnp.float32)
            masked = jnp.where(pattern < slinks[2, t], values, 0.0).astype(jnp.bfloat16)
            col = slinks[3, t]
            back = lax.rem(gx - col // vblocks // ny + nx, nx)
            block = fbuf[back * vblocks + lax.rem(col, vblocks)]
            terms.append(jnp.dot(masked, block, preferred_element_type=jnp.float32))
        for u in range(group):
            t = i * piece + step * group + u
            prefix[t] = terms[u] + prefix[slinks[0, t]]
        return carry

    for i in range(len(held)):
        lax.fori_loop(0, piece // group, functools.partial(multiply, i), 0)

    meta(mate, mate, 0).wait_recv()
    for d in range(1, half):
        remote(mbuf.at[mate], mbuf.at[mate], ms, mr.at[half], (gx, near(d))).start()

    def summed(h, q, v):
        return prefix[slinks[1, (h * 2 + q) * vblocks + v]]

    def beside(u):
        return upper * near_heights + lax.rem(lax.rem(height, near_heights) + u, near_heights)

    def heights(u):
        h = beside(u)
        return (h, nh - 1 - h)

    span = 2 * vblocks
    halves = {}
    for u in [*range(1, near_heights), 0]:
        for w, h in enumerate(heights(u)):
            for v in range(vblocks):
                psend[u * span + w * vblocks + v] = summed(h, 1 - side, v)
        where = pl.ds(u * span, span)
        copy = remote(
            psend.at[where], precv.at[where], ps, pr.at[u], (gx, gy + 1 - 2 * side)
        )
        copy.start()
        halves[u] = copy
    for way in batches[1]:
        send_tiles(*way)

    joins = []
    for u in range(1, near_heights):
        halves[u].wait_recv()
        for w, h in enumerate(heights(u)):
            for v in range(vblocks):
                at = u * span + w * vblocks + v
                asend[at] = summed(h, side, v) + precv[at]
        where = pl.ds(u * span, span)
        copy = remote(
            asend.at[where], arecv.at[where], ps, xr, (gx, beside(u) * 2 + side)
        )
        copy.start()
        joins.append(copy)
    for way in batches[2]:
        send_tiles(*way)

    halves[0].wait_recv()
    if joins:
        landed(arecv.at[pl.ds(span, len(joins) * span)], xr)

    def gathered(w, h, v):
        total = summed(h, side, v) + precv[w * vblocks + v]
        for u in range(1, near_heights):
            total = total + arecv[u * span + w * vblocks + v]
        return total

    mirror = nh - 1 - height
    for v in range(vblocks):
        term = gathered(1, mirror, v)
        peak = jnp.max(jnp.abs(term), axis=0, keepdims=True)
        small = peak < 2.0**-62
        term, peak = term * jnp.where(small, 2.0**64, 1.0), peak * jnp.where(small, 2.0**64, 1.0)
        term = term * jnp.where(peak > 0, 32767.0 / jnp.where(peak > 0, peak, 1.0), 0.0)
        term = (term + jnp.where(term < 0, -0.5, 0.5)).astype(jnp.int32)
        qsend[pl.ds(v * order, order)] = term.astype(jnp.int16)
        ssend[v : v + 1, :] = peak * (1.0 / 32767.0)
        ssend[vblocks + v : vblocks + v + 1, :] = jnp.where(small, 2.0**-64, 1.0)
    owner = (gx, mirror * 2 + side)
    tail = order * LENT // 128
    body, end = pl.ds(0, vblocks * order - tail), pl.ds(vblocks * order - tail, tail)
    lends, carries = (upper > 0) & (side == 0), (upper > 0) & (side == 1)
    partials = [
        remote(ssend, srecv, qs, qr.at[0], owner),
        remote(qsend.at[body], qrecv.at[body], ps, qr.at[1], owner),
    ]
    direct = remote(qsend.at[end], qrecv.at[end], ps, qr.at[1], owner)
    lent = remote(qsend.at[end], carried, ps, cr, (gx, lax.rem(gy + 1, ny)))
    carry_on = remote(carried, qrecv.at[end], cs, qr.at[1], (gx, lax.rem(mirror * 2 + 1 - side, ny)))
    pl.when(lends)(lent.start)

    @pl.when(carries)
    def _():
        lent.wait_recv()
        carry_on.start()

    for copy in partials:
        copy.start()
    pl.when(~lends)(direct.start)
    for way in batches[3]:
        send_tiles(*way)


    own = [gathered(0, height, v) for v in range(vblocks)]
    for d in range(1, half):
        c = near(half - d)
        pl.when(~needed(c))(meta(c, c, d).wait_recv)
    landed(mbuf.at[pl.ds(0, half - 1)], mr.at[half])
    count = [jnp.sum((mbuf[c, 0:1, :] > 0).astype(jnp.int32)) for c in range(ny)]
    first = [jnp.int32(0)]
    for c in range(ny - 1):
        first.append(first[-1] + count[c])
    table_ref[...] = jnp.zeros(table_ref.shape, jnp.int32)
    slot = lax.broadcasted_iota(jnp.int32, (1, 128), 1)
    wanted = slot * ny + gy
    at = jnp.full((1, 128), slots, jnp.int32)
    for c in range(ny):
        offset = c * share + (gy - first[c] + slots * ny) // ny - slots
        here = (wanted >= first[c]) & (wanted < first[c] + count[c])
        at = jnp.where(here, slot + offset, at)
    links[0:1, :] = at
    placing = pltpu.make_async_copy(links, slinks, isem)
    placing.start()
    lane = lax.broadcasted_iota(jnp.int32, (owned, 128), 1)
    line = lax.broadcasted_iota(jnp.int32, (owned, 128), 0)
    wanted = line * ny + gy
    sums = [jnp.zeros((owned, 128), jnp.int32) for _ in range(3)]
    for c in range(ny):
        work = mbuf[c, 0:1, :]
        hit = (lane + first[c] == wanted) & (work > 0)
        for i in range(3):
            sums[i] = sums[i] + jnp.where(hit, mbuf[c, i : i + 1, :], 0)
    for i in range(3):
        column = jnp.sum(sums[i], axis=1, keepdims=True)
        spread = jnp.where(line == lane, jnp.broadcast_to(column, (owned, 128)), 0)
        table_ref[i : i + 1, :] = jnp.sum(spread, axis=0, keepdims=True)

    placing.wait()
    landed(recv.at[pl.ds(0, (ny - 1) * share)], tr)

    def settle(s, carry):
        moved_ref[s] = recv[slinks[0, s]]
        return carry

    lax.fori_loop(0, owned, settle, 0, unroll=4)
    partials[0].wait_recv()
    landed(qrecv, qr.at[1])
    for v in range(vblocks):
        coded = qrecv[pl.ds(v * order, order)].astype(jnp.int32).astype(jnp.float32)
        scale = srecv[v : v + 1, :]
        prod_ref[v] = own[v] + coded * scale * srecv[vblocks + v : vblocks + v + 1, :]
    landed(mbuf.at[pl.ds(0, ny - 1)], ms)
    landed(fbuf.at[pl.ds(0, (nx - 1) * vblocks)], fs)
    landed(stage.at[pl.ds(0, (ny - 1) * share)], ts)
    blocks = (near_heights + len(joins)) * span + vblocks // 2
    landed(prefix.at[pl.ds(0, blocks)], ps)
    partials[0].wait_send()
    pl.when(carries)(carry_on.wait_send)


def deliver(owned, meta_ref, prod_ref, moved_ref, prod_out, moved_out, row_out, col_out, work_out, lists, sems):
    part = owned // 1
    outs = [(prod_ref, prod_out)]
    for i in range(1):
        where = pl.ds(i * part, part)
        outs.append((moved_ref.at[where], moved_out.at[where]))
    for i, ref in enumerate((work_out, row_out, col_out)):
        lists[i] = meta_ref[i, 0:owned]
        outs.append((lists.at[i], ref))
    copies = [pltpu.make_async_copy(*pair, sems.at[i]) for i, pair in enumerate(outs)]
    for copy in copies:
        copy.start()
    for copy in copies:
        copy.wait()


def size(shape, kind):
    total = jnp.dtype(kind).itemsize
    for extent in shape:
        total *= extent
    return total


def on_device(nx, ny, features, tile_vals, tile_row, tile_col, tile_work):
    slots, order = tile_vals.shape[:2]
    width = features.shape[1]
    vblocks = features.shape[0] // order
    owned = slots // 2
    near_heights = ny // 4
    half_blocks = near_heights * 2 * vblocks
    vmem = pl.BlockSpec(memory_space=pltpu.VMEM)
    anywhere = pl.BlockSpec(memory_space=pl.ANY)
    hbm = pl.BlockSpec(memory_space=pltpu.HBM)
    bf, f32, i32 = jnp.bfloat16, jnp.float32, jnp.int32
    dma = pltpu.SemaphoreType.DMA
    buffers = [
        ((slots // 2, order, order), bf),
        ((slots // 2, order, order), bf),
        ((slots, order, order), bf),
        ((slots + 1, order, order), bf),
        ((nx * vblocks, order, width), bf),
        ((ny, 4, 128), i32),
        ((1, 128), i32),
        ((8, 128), i32),
        None,
        ((slots + 1, order, width), f32),
        ((half_blocks, order, width), f32),
        ((half_blocks, order, width), f32),
        ((half_blocks, order, width), f32),
        ((half_blocks, order, width), f32),
        ((vblocks * order, width), jnp.int16),
        ((vblocks * order, width), jnp.int16),
        ((order * LENT // 128, width), jnp.int16),
        ((2 * vblocks, width), f32),
        ((2 * vblocks, width), f32),
    ]
    results = (
        jax.ShapeDtypeStruct((vblocks, order, width), f32),
        jax.ShapeDtypeStruct((owned, order, order), bf),
        jax.ShapeDtypeStruct((8, 128), i32),
    )
    need = sum(size(*b) for b in buffers if b) + sum(size(r.shape, r.dtype) for r in results)
    product, moved, table = pl.pallas_call(
        functools.partial(exchange, nx, ny, slots, vblocks, owned),
        out_shape=results,
        in_specs=[hbm] * 5,
        out_specs=(vmem, vmem, vmem),
        scratch_shapes=[
            pltpu.VMEM(*b) if b else pltpu.SMEM((8, 128), i32) for b in buffers
        ] + [
            pltpu.VMEM((slots,), i32),
            pltpu.VMEM((slots,), i32),
            pltpu.VMEM((slots,), i32),
            pltpu.SemaphoreType.REGULAR((ny,)), pltpu.SemaphoreType.REGULAR,
            dma((2,)), dma, dma((4,)), dma, dma((ny // 2 + 1,)), dma, dma,
            dma, dma, dma, dma((near_heights,)), dma, dma, dma((2,)), dma, dma,
        ],
        compiler_params=pltpu.CompilerParams(
            collective_id=0, has_side_effects=True, vmem_limit_bytes=need + 4 * 2**20
        ),
    )(*(
        pltpu.with_memory_space_constraint(x, pltpu.HBM)
        for x in (
            tile_work, tile_row, tile_col,
            features.reshape(vblocks, order, width), tile_vals,
        )
    ))
    index = jax.ShapeDtypeStruct((owned,), i32)
    product, moved, row, col, work = pl.pallas_call(
        functools.partial(deliver, owned),
        out_shape=(
            jax.ShapeDtypeStruct((vblocks, order, width), f32),
            jax.ShapeDtypeStruct((owned, order, order), bf),
            index, index, index,
        ),
        in_specs=[vmem, vmem, vmem],
        out_specs=(hbm,) * 5,
        scratch_shapes=[pltpu.VMEM((3, owned), i32), dma((4 + 1,))],
        compiler_params=pltpu.CompilerParams(vmem_limit_bytes=4 * 2**20),
    )(table, product, moved)
    return product.reshape(vblocks * order, width), moved, row, col, work


def solution(mesh):
    both = ("gx", "gy")
    return jax.shard_map(
        functools.partial(on_device, mesh.shape["gx"], mesh.shape["gy"]),
        mesh=mesh,
        in_specs=(P(both, None), P(both, None, None), P(both), P(both), P(both)),
        out_specs=(P(both, None), P(both, None, None), P(both), P(both), P(both)),
        check_vma=False,
    )
```
